32 devices in a mesh: dp: 4 (over x, y), tp: 8 (over z, core).
Axes of the slice: x: 2, y: 2, z: 4, core: 2. Of those that a mesh axis runs over, the one named last changes fastest.
Arguments:
- x: bfloat16 [8192, 3072], P('dp'), parts along dimension 0
- w_gate: bfloat16 [3072, 8192], P(None, 'tp')
- w_up: bfloat16 [3072, 8192], P(None, 'tp')
- w_down: bfloat16 [8192, 3072], P('tp')
Outputs:
- output: bfloat16 [8192, 3072], P('dp'), parts along dimension 0
There are 4 independent parts. The reference program is written for one: setup_inputs(seed, part) draws one part's arguments, and reference() takes and returns one part's arrays. A program takes and returns all parts, laid end to end along the dimension named above; an argument that names none is the same for every part.
All inputs are finite; a program needn't handle non-finite values.
Results may differ from the reference program's by a relative error of at most 0.016.
Values are sent between devices in bfloat16 or wider.
A program may use at most 2 GiB of HBM per device.

```python
import jax
import jax.numpy as jnp

ROWS = 2048
D = 3072
FF = 8192


def setup_inputs(seed: int = 0, part: int = 0) -> dict:
    kx, kg, ku, kd = jax.random.split(jax.random.key(seed), 4)
    drawn = {
        "x": jax.random.normal(jax.random.fold_in(kx, part), (ROWS, D), jnp.float32),
        "w_gate": jax.random.normal(kg, (D, FF), jnp.float32) * D**-0.5,
        "w_up": jax.random.normal(ku, (D, FF), jnp.float32) * D**-0.5,
        "w_down": jax.random.normal(kd, (FF, D), jnp.float32) * FF**-0.5,
    }
    return {k: v.astype(jnp.bfloat16) for k, v in drawn.items()}


def reference(x, w_gate, w_up, w_down):
    gate = jnp.dot(x, w_gate, preferred_element_type=jnp.float32)
    up = jnp.dot(x, w_up, preferred_element_type=jnp.float32)
    hidden = (jax.nn.silu(gate) * up).astype(jnp.bfloat16)
    return jnp.dot(hidden, w_down, preferred_element_type=jnp.float32).astype(jnp.bfloat16)
```

```python
import functools

import jax
import jax.numpy as jnp
from jax import lax
from jax.experimental import pallas as pl
from jax.experimental.pallas import tpu as pltpu
from jax.sharding import PartitionSpec as P

MESH = pl.DeviceIdType.MESH
CHIPS = 4
CHUNK = 128
TILES = 4
RING = 8
STAGE = 4
SUM_LAG = (1, 3, 6, 3)
DONE_LAG = (12, 6, 12, 12)


def by_place(place, values):
    result = jnp.int32(values[-1])
    for k in range(len(values) - 1):
        result = jnp.where(place == k, jnp.int32(values[k]), result)
    return result


def kernel(
    chunk, tiles, x_hbm, gate_hbm, up_hbm, down_hbm, y_hbm,
    gate_w, up_w, down_w, x_buf, hidden, own, stage, theirs, low, high, sums,
    x_sem, gate_sem, up_sem, down_sem, stage_sem, theirs_sem, low_sem, high_sem,
    sum_sem, spread_sem, pass_sem, y_sem, give_sem, take_sem,
):
    rows, depth = x_hbm.shape
    units = gate_hbm.shape[1]
    half = rows // 2
    chunks = half // chunk
    pieces = chunks * tiles
    unit_tile = units // tiles
    col_tile = depth // tiles

    me = lax.axis_index("tp")
    chip, core = me // 2, me % 2
    place = jnp.where(core == 1, chip, CHIPS - 1 - chip)

    def at_place(k):
        return {"tp": jnp.where(core == 1, k, CHIPS - 1 - k) * 2 + core}

    other = {"tp": me + 1 - 2 * core}
    before, after = at_place(place - 1), at_place(place + 1)
    inner = jnp.logical_or(place == 1, place == 2)

    barrier = pltpu.get_barrier_semaphore()
    pl.semaphore_signal(barrier, inc=1, device_id=other, device_id_type=MESH)

    @pl.when(place > 0)
    def _():
        pl.semaphore_signal(barrier, inc=1, device_id=before, device_id_type=MESH)

    @pl.when(place < CHIPS - 1)
    def _():
        pl.semaphore_signal(barrier, inc=1, device_id=after, device_id_type=MESH)

    def x_rows(which, c):
        return x_hbm.at[pl.ds(pl.multiple_of(which * half + c * chunk, chunk), chunk), :]

    def fetch_x(c):
        slot = lax.rem(c, 2)
        pltpu.make_async_copy(x_rows(core, c), x_buf.at[slot, pl.ds(0, chunk)], x_sem.at[slot]).start()
        pltpu.make_async_copy(x_rows(1 - core, c), x_buf.at[slot, pl.ds(chunk, chunk)], x_sem.at[slot]).start()

    def wait_x(c):
        slot = lax.rem(c, 2)
        pltpu.make_async_copy(x_hbm.at[pl.ds(0, 2 * chunk), :], x_buf.at[slot], x_sem.at[slot]).wait()

    def unit_slice(t):
        return slice(t * unit_tile, (t + 1) * unit_tile)

    def col_slice(t):
        return slice(t * col_tile, (t + 1) * col_tile)

    def gate_copy(t):
        return pltpu.make_async_copy(gate_hbm.at[:, unit_slice(t)], gate_w.at[:, unit_slice(t)], gate_sem.at[t])

    def up_copy(t):
        return pltpu.make_async_copy(up_hbm.at[:, unit_slice(t)], up_w.at[:, unit_slice(t)], up_sem.at[t])

    def down_copy(t):
        return pltpu.make_async_copy(down_hbm.at[:, col_slice(t)], down_w.at[:, col_slice(t)], down_sem.at[t])

    fetch_x(0)
    for t in range(tiles):
        gate_copy(t).start()
        up_copy(t).start()
    fetch_x(1)
    for t in range(tiles):
        down_copy(t).start()

    def project(c, t):
        slot = lax.rem(c, 2)
        xs = x_buf[slot]
        gate = jnp.dot(xs, gate_w[:, unit_slice(t)], preferred_element_type=jnp.float32)
        up = jnp.dot(xs, up_w[:, unit_slice(t)], preferred_element_type=jnp.float32)
        hidden[slot, :, unit_slice(t)] = (jax.nn.silu(gate) * up).astype(jnp.bfloat16)

    def stage_copy(i):
        slot = lax.rem(i, STAGE)
        return pltpu.make_async_remote_copy(
            src_ref=stage.at[slot], dst_ref=theirs.at[i], send_sem=stage_sem.at[slot], recv_sem=theirs_sem.at[i],
            device_id=other, device_id_type=MESH,
        )

    def terms(c, t):
        i = c * tiles + t
        term = jnp.dot(hidden[lax.rem(c, 2)], down_w[:, col_slice(t)], preferred_element_type=jnp.float32)

        @pl.when(i >= STAGE)
        def _():
            stage_copy(i - STAGE).wait_send()

        stage[lax.rem(i, STAGE)] = term[chunk:].astype(jnp.bfloat16)
        stage_copy(i).start()
        own[lax.rem(i, RING)] = term[:chunk]

    def low_copy(p):
        return pltpu.make_async_remote_copy(
            src_ref=sums.at[p], dst_ref=low.at[p], send_sem=sum_sem, recv_sem=low_sem.at[p],
            device_id=after, device_id_type=MESH,
        )

    def high_copy(p):
        return pltpu.make_async_remote_copy(
            src_ref=sums.at[p], dst_ref=high.at[p], send_sem=sum_sem, recv_sem=high_sem.at[p],
            device_id=before, device_id_type=MESH,
        )

    def spread_copy(p):
        return pltpu.make_async_remote_copy(
            src_ref=sums.at[p], dst_ref=high.at[p], send_sem=spread_sem, recv_sem=high_sem.at[p],
            device_id=after, device_id_type=MESH,
        )

    def pass_copy(p):
        return pltpu.make_async_remote_copy(
            src_ref=high.at[p], dst_ref=high.at[p], send_sem=pass_sem, recv_sem=high_sem.at[p],
            device_id=before, device_id_type=MESH,
        )

    def deliver(src, p):
        c, t = p // tiles, lax.rem(p, tiles)
        block = y_hbm.at[
            pl.ds(pl.multiple_of(core * half + c * chunk, chunk), chunk),
            pl.ds(pl.multiple_of(t * col_tile, col_tile), col_tile),
        ]
        pltpu.make_async_remote_copy(
            src_ref=src, dst_ref=block, send_sem=give_sem, recv_sem=take_sem, device_id=other, device_id_type=MESH,
        ).start()
        pltpu.make_async_copy(src, block, y_sem).start()

    def combine(p):
        pltpu.make_async_copy(theirs.at[p], theirs.at[p], theirs_sem.at[p]).wait()

        def here():
            return own[lax.rem(p, RING)] + theirs[p].astype(jnp.float32)

        @pl.when(jnp.logical_not(inner))
        def _():
            sums[p] = here().astype(jnp.bfloat16)

        @pl.when(inner)
        def _():
            pltpu.make_async_copy(low.at[p], low.at[p], low_sem.at[p]).wait()

        @pl.when(place == 1)
        def _():
            sums[p] = (here() + low[p].astype(jnp.float32)).astype(jnp.bfloat16)

        @pl.when(place == 2)
        def _():
            pltpu.make_async_copy(high.at[p], high.at[p], high_sem.at[p]).wait()
            sums[p] = (here() + low[p].astype(jnp.float32) + high[p].astype(jnp.float32)).astype(jnp.bfloat16)

        @pl.when(place < 2)
        def _():
            low_copy(p).start()

        @pl.when(place >= 2)
        def _():
            high_copy(p).start()

        @pl.when(place == 2)
        def _():
            spread_copy(p).start()
            deliver(sums.at[p], p)

    def finish(p):
        pltpu.make_async_copy(high.at[p], high.at[p], high_sem.at[p]).wait()

        @pl.when(place == 1)
        def _():
            pass_copy(p).start()

        deliver(high.at[p], p)

    sum_lag = by_place(place, SUM_LAG)
    done_lag = by_place(place, DONE_LAG)

    def trail(i):
        p = i - sum_lag

        @pl.when(jnp.logical_and(p >= 0, p < pieces))
        def _():
            combine(p)

        d = i - done_lag

        @pl.when(jnp.logical_and(jnp.logical_and(d >= 0, d < pieces), place != 2))
        def _():
            finish(d)

    wait_x(0)
    for t in range(tiles):
        gate_copy(t).wait()
        up_copy(t).wait()
        project(0, t)
    for t in range(tiles):
        down_copy(t).wait()

    pl.semaphore_wait(barrier, jnp.where(inner, 3, 2))

    @pl.loop(0, chunks)
    def _(c):
        @pl.when(c + 2 < chunks)
        def _():
            fetch_x(c + 2)

        @pl.when(c + 1 < chunks)
        def _():
            wait_x(c + 1)

        for t in range(tiles):
            terms(c, t)

            @pl.when(c + 1 < chunks)
            def _():
                project(c + 1, t)

            trail(c * tiles + t)

    @pl.loop(pieces, pieces + max(SUM_LAG + DONE_LAG))
    def _(i):
        trail(i)

    for k in range(STAGE):
        stage_copy(pieces - STAGE + k).wait_send()
    pltpu.make_async_copy(sums, sums, sum_sem).wait()

    @pl.when(place == 2)
    def _():
        pltpu.make_async_copy(sums, sums, spread_sem).wait()

    @pl.when(place == 1)
    def _():
        pltpu.make_async_copy(high, high, pass_sem).wait()

    pltpu.make_async_copy(sums, sums, y_sem).wait()
    pltpu.make_async_copy(sums, sums, give_sem).wait()
    pltpu.make_async_copy(sums, sums, take_sem).wait()


def block(x, w_gate, w_up, w_down, chunk=CHUNK, tiles=TILES):
    rows, depth = x.shape
    units = w_gate.shape[1]
    pieces = rows // 2 // chunk * tiles
    piece = (chunk, depth // tiles)
    buffers = pltpu.VMEM((pieces,) + piece, jnp.bfloat16)
    dma = pltpu.SemaphoreType.DMA
    anywhere = pl.BlockSpec(memory_space=pl.ANY)
    return pl.pallas_call(
        functools.partial(kernel, chunk, tiles),
        out_shape=jax.ShapeDtypeStruct((rows, depth), jnp.bfloat16),
        in_specs=[anywhere] * 4,
        out_specs=anywhere,
        scratch_shapes=[
            pltpu.VMEM((depth, units), jnp.bfloat16),
            pltpu.VMEM((depth, units), jnp.bfloat16),
            pltpu.VMEM((units, depth), jnp.bfloat16),
            pltpu.VMEM((2, 2 * chunk, depth), jnp.bfloat16),
            pltpu.VMEM((2, 2 * chunk, units), jnp.bfloat16),
            pltpu.VMEM((RING,) + piece, jnp.float32),
            pltpu.VMEM((STAGE,) + piece, jnp.bfloat16),
            buffers, buffers, buffers, buffers,
            dma((2,)), dma((tiles,)), dma((tiles,)), dma((tiles,)), dma((STAGE,)),
            dma((pieces,)), dma((pieces,)), dma((pieces,)),
            dma, dma, dma, dma, dma, dma,
        ],
        compiler_params=pltpu.CompilerParams(
            collective_id=0, has_side_effects=True, vmem_limit_bytes=66_000_000
        ),
    )(x, w_gate, w_up, w_down)


def solution(mesh):
    return jax.shard_map(
        block,
        mesh=mesh,
        in_specs=(P("dp", None), P(None, "tp"), P(None, "tp"), P("tp", None)),
        out_specs=P("dp", None),
        check_vma=False,
    )
```

```python
import functools

import jax
import jax.numpy as jnp
from jax import lax
from jax.experimental import pallas as pl
from jax.experimental.pallas import tpu as pltpu
from jax.sharding import PartitionSpec as P

MESH = pl.DeviceIdType.MESH
CHIPS = 4
CHUNK = 64
TILES = 4
RING = 16
STAGE = 4
SUM_LAG = (1, 4, 10, 5)
DONE_LAG = (24, 9, 24, 24)


def by_place(place, values):
    result = jnp.int32(values[-1])
    for k in range(len(values) - 1):
        result = jnp.where(place == k, jnp.int32(values[k]), result)
    return result


def kernel(
    chunk, tiles, x_hbm, gate_hbm, up_hbm, down_hbm, y_hbm,
    gate_w, up_w, down_w, x_buf, hidden, own, stage, theirs, low, high, sums,
    x_sem, gate_sem, up_sem, down_sem, stage_sem, theirs_sem, low_sem, high_sem,
    sum_sem, spread_sem, pass_sem, y_sem, give_sem, take_sem,
):
    rows, depth = x_hbm.shape
    units = gate_hbm.shape[1]
    half = rows // 2
    chunks = half // chunk
    pieces = chunks * tiles
    unit_tile = units // tiles
    col_tile = depth // tiles

    me = lax.axis_index("tp")
    chip, core = me // 2, me % 2
    place = jnp.where(core == 1, chip, CHIPS - 1 - chip)

    def at_place(k):
        return {"tp": jnp.where(core == 1, k, CHIPS - 1 - k) * 2 + core}

    other = {"tp": me + 1 - 2 * core}
    before, after = at_place(place - 1), at_place(place + 1)
    inner = jnp.logical_or(place == 1, place == 2)

    barrier = pltpu.get_barrier_semaphore()
    pl.semaphore_signal(barrier, inc=1, device_id=other, device_id_type=MESH)

    @pl.when(place > 0)
    def _():
        pl.semaphore_signal(barrier, inc=1, device_id=before, device_id_type=MESH)

    @pl.when(place < CHIPS - 1)
    def _():
        pl.semaphore_signal(barrier, inc=1, device_id=after, device_id_type=MESH)

    def x_rows(which, c):
        return x_hbm.at[pl.ds(pl.multiple_of(which * half + c * chunk, chunk), chunk), :]

    def fetch_x(c):
        slot = lax.rem(c, 2)
        pltpu.make_async_copy(x_rows(core, c), x_buf.at[slot, pl.ds(0, chunk)], x_sem.at[slot]).start()
        pltpu.make_async_copy(x_rows(1 - core, c), x_buf.at[slot, pl.ds(chunk, chunk)], x_sem.at[slot]).start()

    def wait_x(c):
        slot = lax.rem(c, 2)
        pltpu.make_async_copy(x_hbm.at[pl.ds(0, 2 * chunk), :], x_buf.at[slot], x_sem.at[slot]).wait()

    def unit_slice(t):
        return slice(t * unit_tile, (t + 1) * unit_tile)

    def col_slice(t):
        return slice(t * col_tile, (t + 1) * col_tile)

    def gate_copy(t):
        return pltpu.make_async_copy(gate_hbm.at[:, unit_slice(t)], gate_w.at[:, unit_slice(t)], gate_sem.at[t])

    def up_copy(t):
        return pltpu.make_async_copy(up_hbm.at[:, unit_slice(t)], up_w.at[:, unit_slice(t)], up_sem.at[t])

    def down_copy(t):
        return pltpu.make_async_copy(down_hbm.at[:, col_slice(t)], down_w.at[:, col_slice(t)], down_sem.at[t])

    fetch_x(0)
    for t in range(tiles):
        gate_copy(t).start()
        up_copy(t).start()
    fetch_x(1)
    for t in range(tiles):
        down_copy(t).start()

    def project(c, t):
        slot = lax.rem(c, 2)
        xs = x_buf[slot]
        gate = jnp.dot(xs, gate_w[:, unit_slice(t)], preferred_element_type=jnp.float32)
        up = jnp.dot(xs, up_w[:, unit_slice(t)], preferred_element_type=jnp.float32)
        hidden[slot, :, unit_slice(t)] = (jax.nn.silu(gate) * up).astype(jnp.bfloat16)

    def stage_copy(i):
        slot = lax.rem(i, STAGE)
        return pltpu.make_async_remote_copy(
            src_ref=stage.at[slot], dst_ref=theirs.at[i], send_sem=stage_sem.at[slot], recv_sem=theirs_sem.at[i],
            device_id=other, device_id_type=MESH,
        )

    def terms(c, t):
        i = c * tiles + t
        term = jnp.dot(hidden[lax.rem(c, 2)], down_w[:, col_slice(t)], preferred_element_type=jnp.float32)

        @pl.when(i >= STAGE)
        def _():
            stage_copy(i - STAGE).wait_send()

        stage[lax.rem(i, STAGE)] = term[chunk:].astype(jnp.bfloat16)
        stage_copy(i).start()
        own[lax.rem(i, RING)] = term[:chunk]

    def low_copy(p):
        return pltpu.make_async_remote_copy(
            src_ref=sums.at[p], dst_ref=low.at[p], send_sem=sum_sem, recv_sem=low_sem.at[p],
            device_id=after, device_id_type=MESH,
        )

    def high_copy(p):
        return pltpu.make_async_remote_copy(
            src_ref=sums.at[p], dst_ref=high.at[p], send_sem=sum_sem, recv_sem=high_sem.at[p],
            device_id=before, device_id_type=MESH,
        )

    def spread_copy(p):
        return pltpu.make_async_remote_copy(
            src_ref=sums.at[p], dst_ref=high.at[p], send_sem=spread_sem, recv_sem=high_sem.at[p],
            device_id=after, device_id_type=MESH,
        )

    def pass_copy(p):
        return pltpu.make_async_remote_copy(
            src_ref=high.at[p], dst_ref=high.at[p], send_sem=pass_sem, recv_sem=high_sem.at[p],
            device_id=before, device_id_type=MESH,
        )

    def deliver(src, p):
        c, t = p // tiles, lax.rem(p, tiles)
        block = y_hbm.at[
            pl.ds(pl.multiple_of(core * half + c * chunk, chunk), chunk),
            pl.ds(pl.multiple_of(t * col_tile, col_tile), col_tile),
        ]
        pltpu.make_async_remote_copy(
            src_ref=src, dst_ref=block, send_sem=give_sem, recv_sem=take_sem, device_id=other, device_id_type=MESH,
        ).start()
        pltpu.make_async_copy(src, block, y_sem).start()

    def combine(p):
        pltpu.make_async_copy(theirs.at[p], theirs.at[p], theirs_sem.at[p]).wait()

        def here():
            return own[lax.rem(p, RING)] + theirs[p].astype(jnp.float32)

        @pl.when(jnp.logical_not(inner))
        def _():
            sums[p] = here().astype(jnp.bfloat16)

        @pl.when(inner)
        def _():
            pltpu.make_async_copy(low.at[p], low.at[p], low_sem.at[p]).wait()

        @pl.when(place == 1)
        def _():
            sums[p] = (here() + low[p].astype(jnp.float32)).astype(jnp.bfloat16)

        @pl.when(place == 2)
        def _():
            pltpu.make_async_copy(high.at[p], high.at[p], high_sem.at[p]).wait()
            sums[p] = (here() + low[p].astype(jnp.float32) + high[p].astype(jnp.float32)).astype(jnp.bfloat16)

        @pl.when(place < 2)
        def _():
            low_copy(p).start()

        @pl.when(place >= 2)
        def _():
            high_copy(p).start()

        @pl.when(place == 2)
        def _():
            spread_copy(p).start()
            deliver(sums.at[p], p)

    def finish(p):
        pltpu.make_async_copy(high.at[p], high.at[p], high_sem.at[p]).wait()

        @pl.when(place == 1)
        def _():
            pass_copy(p).start()

        deliver(high.at[p], p)

    sum_lag = by_place(place, SUM_LAG)
    done_lag = by_place(place, DONE_LAG)

    def trail(i):
        p = i - sum_lag

        @pl.when(jnp.logical_and(p >= 0, p < pieces))
        def _():
            combine(p)

        d = i - done_lag

        @pl.when(jnp.logical_and(jnp.logical_and(d >= 0, d < pieces), place != 2))
        def _():
            finish(d)

    wait_x(0)
    for t in range(tiles):
        gate_copy(t).wait()
        up_copy(t).wait()
        project(0, t)
    for t in range(tiles):
        down_copy(t).wait()

    pl.semaphore_wait(barrier, jnp.where(inner, 3, 2))

    @pl.loop(0, chunks)
    def _(c):
        @pl.when(c + 2 < chunks)
        def _():
            fetch_x(c + 2)

        @pl.when(c + 1 < chunks)
        def _():
            wait_x(c + 1)

        for t in range(tiles):
            terms(c, t)

            @pl.when(c + 1 < chunks)
            def _():
                project(c + 1, t)

            trail(c * tiles + t)

    @pl.loop(pieces, pieces + max(SUM_LAG + DONE_LAG))
    def _(i):
        trail(i)

    for k in range(STAGE):
        stage_copy(pieces - STAGE + k).wait_send()
    pltpu.make_async_copy(sums, sums, sum_sem).wait()

    @pl.when(place == 2)
    def _():
        pltpu.make_async_copy(sums, sums, spread_sem).wait()

    @pl.when(place == 1)
    def _():
        pltpu.make_async_copy(high, high, pass_sem).wait()

    pltpu.make_async_copy(sums, sums, y_sem).wait()
    pltpu.make_async_copy(sums, sums, give_sem).wait()
    pltpu.make_async_copy(sums, sums, take_sem).wait()


def block(x, w_gate, w_up, w_down, chunk=CHUNK, tiles=TILES):
    rows, depth = x.shape
    units = w_gate.shape[1]
    pieces = rows // 2 // chunk * tiles
    piece = (chunk, depth // tiles)
    buffers = pltpu.VMEM((pieces,) + piece, jnp.bfloat16)
    dma = pltpu.SemaphoreType.DMA
    anywhere = pl.BlockSpec(memory_space=pl.ANY)
    return pl.pallas_call(
        functools.partial(kernel, chunk, tiles),
        out_shape=jax.ShapeDtypeStruct((rows, depth), jnp.bfloat16),
        in_specs=[anywhere] * 4,
        out_specs=anywhere,
        scratch_shapes=[
            pltpu.VMEM((depth, units), jnp.bfloat16),
            pltpu.VMEM((depth, units), jnp.bfloat16),
            pltpu.VMEM((units, depth), jnp.bfloat16),
            pltpu.VMEM((2, 2 * chunk, depth), jnp.bfloat16),
            pltpu.VMEM((2, 2 * chunk, units), jnp.bfloat16),
            pltpu.VMEM((RING,) + piece, jnp.float32),
            pltpu.VMEM((STAGE,) + piece, jnp.bfloat16),
            buffers, buffers, buffers, buffers,
            dma((2,)), dma((tiles,)), dma((tiles,)), dma((tiles,)), dma((STAGE,)),
            dma((pieces,)), dma((pieces,)), dma((pieces,)),
            dma, dma, dma, dma, dma, dma,
        ],
        compiler_params=pltpu.CompilerParams(
            collective_id=0, has_side_effects=True, vmem_limit_bytes=66_000_000
        ),
    )(x, w_gate, w_up, w_down)


def solution(mesh):
    return jax.shard_map(
        block,
        mesh=mesh,
        in_specs=(P("dp", None), P(None, "tp"), P(None, "tp"), P("tp", None)),
        out_specs=P("dp", None),
        check_vma=False,
    )
```

```python
import functools

import jax
import jax.numpy as jnp
from jax import lax
from jax.experimental import pallas as pl
from jax.experimental.pallas import tpu as pltpu
from jax.sharding import PartitionSpec as P

MESH = pl.DeviceIdType.MESH
CHIPS = 4
CHUNK = 64
TILES = 4
RING = 16
STAGE = 4
OUT_COPIES = 16
OUT_LIMIT = 1_000_000
SUM_LAG = (1, 4, 10, 5)
DONE_LAG = (24, 9, 24, 24)


def by_place(place, values):
    result = jnp.int32(values[-1])
    for k in range(len(values) - 1):
        result = jnp.where(place == k, jnp.int32(values[k]), result)
    return result


def kernel(
    chunk, tiles, x_hbm, gate_hbm, up_hbm, down_hbm, y_hbm,
    gate_w, up_w, down_w, x_buf, hidden, own, stage, theirs, low, high, sums,
    x_sem, gate_sem, up_sem, down_sem, stage_sem, theirs_sem, low_sem, high_sem,
    sum_sem, spread_sem, pass_sem, y_sem, give_sem, take_sem,
):
    rows, depth = x_hbm.shape
    units = gate_hbm.shape[1]
    half = rows // 2
    chunks = half // chunk
    pieces = chunks * tiles
    unit_tile = units // tiles
    col_tile = depth // tiles

    me = lax.axis_index("tp")
    chip, core = me // 2, me % 2
    place = jnp.where(core == 1, chip, CHIPS - 1 - chip)

    def at_place(k):
        return {"tp": jnp.where(core == 1, k, CHIPS - 1 - k) * 2 + core}

    other = {"tp": me + 1 - 2 * core}
    before, after = at_place(place - 1), at_place(place + 1)
    inner = jnp.logical_or(place == 1, place == 2)

    barrier = pltpu.get_barrier_semaphore()
    pl.semaphore_signal(barrier, inc=1, device_id=other, device_id_type=MESH)

    @pl.when(place > 0)
    def _():
        pl.semaphore_signal(barrier, inc=1, device_id=before, device_id_type=MESH)

    @pl.when(place < CHIPS - 1)
    def _():
        pl.semaphore_signal(barrier, inc=1, device_id=after, device_id_type=MESH)

    def x_rows(which, c):
        return x_hbm.at[pl.ds(pl.multiple_of(which * half + c * chunk, chunk), chunk), :]

    def fetch_x(c):
        slot = lax.rem(c, 2)
        pltpu.make_async_copy(x_rows(core, c), x_buf.at[slot, pl.ds(0, chunk)], x_sem.at[slot]).start()
        pltpu.make_async_copy(x_rows(1 - core, c), x_buf.at[slot, pl.ds(chunk, chunk)], x_sem.at[slot]).start()

    def wait_x(c):
        slot = lax.rem(c, 2)
        pltpu.make_async_copy(x_hbm.at[pl.ds(0, 2 * chunk), :], x_buf.at[slot], x_sem.at[slot]).wait()

    def unit_slice(t):
        return slice(t * unit_tile, (t + 1) * unit_tile)

    def col_slice(t):
        return slice(t * col_tile, (t + 1) * col_tile)

    def gate_copy(t):
        return pltpu.make_async_copy(gate_hbm.at[:, unit_slice(t)], gate_w.at[:, unit_slice(t)], gate_sem.at[t])

    def up_copy(t):
        return pltpu.make_async_copy(up_hbm.at[:, unit_slice(t)], up_w.at[:, unit_slice(t)], up_sem.at[t])

    def down_copy(t):
        return pltpu.make_async_copy(down_hbm.at[:, col_slice(t)], down_w.at[:, col_slice(t)], down_sem.at[t])

    fetch_x(0)
    for t in range(tiles):
        gate_copy(t).start()
        up_copy(t).start()
    fetch_x(1)
    for t in range(tiles):
        down_copy(t).start()

    def project(c, t):
        slot = lax.rem(c, 2)
        xs = x_buf[slot]
        gate = jnp.dot(xs, gate_w[:, unit_slice(t)], preferred_element_type=jnp.float32)
        up = jnp.dot(xs, up_w[:, unit_slice(t)], preferred_element_type=jnp.float32)
        hidden[slot, :, unit_slice(t)] = (jax.nn.silu(gate) * up).astype(jnp.bfloat16)

    def stage_copy(i):
        slot = lax.rem(i, STAGE)
        return pltpu.make_async_remote_copy(
            src_ref=stage.at[slot], dst_ref=theirs.at[i], send_sem=stage_sem.at[slot], recv_sem=theirs_sem.at[i],
            device_id=other, device_id_type=MESH,
        )

    def terms(c, t):
        i = c * tiles + t
        term = jnp.dot(hidden[lax.rem(c, 2)], down_w[:, col_slice(t)], preferred_element_type=jnp.float32)

        @pl.when(i >= STAGE)
        def _():
            stage_copy(i - STAGE).wait_send()

        stage[lax.rem(i, STAGE)] = term[chunk:].astype(jnp.bfloat16)
        stage_copy(i).start()
        own[lax.rem(i, RING)] = term[:chunk]

    def low_copy(p):
        return pltpu.make_async_remote_copy(
            src_ref=sums.at[p], dst_ref=low.at[p], send_sem=sum_sem, recv_sem=low_sem.at[p],
            device_id=after, device_id_type=MESH,
        )

    def high_copy(p):
        return pltpu.make_async_remote_copy(
            src_ref=sums.at[p], dst_ref=high.at[p], send_sem=sum_sem, recv_sem=high_sem.at[p],
            device_id=before, device_id_type=MESH,
        )

    def spread_copy(p):
        return pltpu.make_async_remote_copy(
            src_ref=sums.at[p], dst_ref=high.at[p], send_sem=spread_sem, recv_sem=high_sem.at[p],
            device_id=after, device_id_type=MESH,
        )

    def pass_copy(p):
        return pltpu.make_async_remote_copy(
            src_ref=high.at[p], dst_ref=high.at[p], send_sem=pass_sem, recv_sem=high_sem.at[p],
            device_id=before, device_id_type=MESH,
        )

    def deliver(src, p):
        c, t = p // tiles, lax.rem(p, tiles)
        block = y_hbm.at[
            pl.ds(pl.multiple_of(core * half + c * chunk, chunk), chunk),
            pl.ds(pl.multiple_of(t * col_tile, col_tile), col_tile),
        ]
        pltpu.make_async_remote_copy(
            src_ref=src, dst_ref=block, send_sem=give_sem, recv_sem=take_sem, device_id=other, device_id_type=MESH,
        ).start()
        pltpu.make_async_copy(src, block, y_sem).start()

    def combine(p):
        pltpu.make_async_copy(theirs.at[p], theirs.at[p], theirs_sem.at[p]).wait()

        def here():
            return own[lax.rem(p, RING)] + theirs[p].astype(jnp.float32)

        @pl.when(jnp.logical_not(inner))
        def _():
            sums[p] = here().astype(jnp.bfloat16)

        @pl.when(inner)
        def _():
            pltpu.make_async_copy(low.at[p], low.at[p], low_sem.at[p]).wait()

        @pl.when(place == 1)
        def _():
            sums[p] = (here() + low[p].astype(jnp.float32)).astype(jnp.bfloat16)

        @pl.when(place == 2)
        def _():
            pltpu.make_async_copy(high.at[p], high.at[p], high_sem.at[p]).wait()
            sums[p] = (here() + low[p].astype(jnp.float32) + high[p].astype(jnp.float32)).astype(jnp.bfloat16)

        @pl.when(place < 2)
        def _():
            low_copy(p).start()

        @pl.when(place >= 2)
        def _():
            high_copy(p).start()

        @pl.when(place == 2)
        def _():
            spread_copy(p).start()
            deliver(sums.at[p], p)

    def finish(p):
        pltpu.make_async_copy(high.at[p], high.at[p], high_sem.at[p]).wait()

        @pl.when(place == 1)
        def _():
            pass_copy(p).start()

        deliver(high.at[p], p)

    sum_lag = by_place(place, SUM_LAG)
    done_lag = by_place(place, DONE_LAG)

    def trail(i):
        p = i - sum_lag

        @pl.when(jnp.logical_and(p >= 0, p < pieces))
        def _():
            combine(p)

        d = i - done_lag

        @pl.when(jnp.logical_and(jnp.logical_and(d >= 0, d < pieces), place != 2))
        def _():
            finish(d)

    wait_x(0)
    for t in range(tiles):
        gate_copy(t).wait()
        up_copy(t).wait()
        project(0, t)
    for t in range(tiles):
        down_copy(t).wait()

    pl.semaphore_wait(barrier, jnp.where(inner, 3, 2))

    @pl.loop(0, chunks)
    def _(c):
        @pl.when(c + 2 < chunks)
        def _():
            fetch_x(c + 2)

        @pl.when(c + 1 < chunks)
        def _():
            wait_x(c + 1)

        for t in range(tiles):
            terms(c, t)

            @pl.when(c + 1 < chunks)
            def _():
                project(c + 1, t)

            trail(c * tiles + t)

    @pl.loop(pieces, pieces + max(SUM_LAG + DONE_LAG))
    def _(i):
        trail(i)

    for k in range(STAGE):
        stage_copy(pieces - STAGE + k).wait_send()
    pltpu.make_async_copy(sums, sums, sum_sem).wait()

    @pl.when(place == 2)
    def _():
        pltpu.make_async_copy(sums, sums, spread_sem).wait()

    @pl.when(place == 1)
    def _():
        pltpu.make_async_copy(high, high, pass_sem).wait()

    pltpu.make_async_copy(sums, sums, y_sem).wait()
    pltpu.make_async_copy(sums, sums, give_sem).wait()
    pltpu.make_async_copy(sums, sums, take_sem).wait()


def put_out(y_vmem, y_hbm, sem):
    rows = y_vmem.shape[0] // OUT_COPIES
    for k in range(OUT_COPIES):
        part = pl.ds(k * rows, rows)
        pltpu.make_async_copy(y_vmem.at[part], y_hbm.at[part], sem).start()
    pltpu.make_async_copy(y_vmem, y_hbm, sem).wait()


def block(x, w_gate, w_up, w_down, chunk=CHUNK, tiles=TILES):
    rows, depth = x.shape
    units = w_gate.shape[1]
    pieces = rows // 2 // chunk * tiles
    piece = (chunk, depth // tiles)
    buffers = pltpu.VMEM((pieces,) + piece, jnp.bfloat16)
    dma = pltpu.SemaphoreType.DMA
    anywhere = pl.BlockSpec(memory_space=pl.ANY)
    y = pl.pallas_call(
        functools.partial(kernel, chunk, tiles),
        out_shape=pltpu.VMEM((rows, depth), jnp.bfloat16),
        in_specs=[anywhere] * 4,
        out_specs=anywhere,
        scratch_shapes=[
            pltpu.VMEM((depth, units), jnp.bfloat16),
            pltpu.VMEM((depth, units), jnp.bfloat16),
            pltpu.VMEM((units, depth), jnp.bfloat16),
            pltpu.VMEM((2, 2 * chunk, depth), jnp.bfloat16),
            pltpu.VMEM((2, 2 * chunk, units), jnp.bfloat16),
            pltpu.VMEM((RING,) + piece, jnp.float32),
            pltpu.VMEM((STAGE,) + piece, jnp.bfloat16),
            buffers, buffers, buffers, buffers,
            dma((2,)), dma((tiles,)), dma((tiles,)), dma((tiles,)), dma((STAGE,)),
            dma((pieces,)), dma((pieces,)), dma((pieces,)),
            dma, dma, dma, dma, dma, dma,
        ],
        compiler_params=pltpu.CompilerParams(
            collective_id=0, has_side_effects=True, vmem_limit_bytes=54_000_000
        ),
    )(x, w_gate, w_up, w_down)
    return pl.pallas_call(
        put_out,
        out_shape=jax.ShapeDtypeStruct((rows, depth), jnp.bfloat16),
        in_specs=[anywhere],
        out_specs=anywhere,
        scratch_shapes=[dma],
        compiler_params=pltpu.CompilerParams(vmem_limit_bytes=OUT_LIMIT),
    )(y)


def solution(mesh):
    return jax.shard_map(
        block,
        mesh=mesh,
        in_specs=(P("dp", None), P(None, "tp"), P(None, "tp"), P("tp", None)),
        out_specs=P("dp", None),
        check_vma=False,
    )
```

```python
import functools

import jax
import jax.numpy as jnp
from jax import lax
from jax.experimental import pallas as pl
from jax.experimental.pallas import tpu as pltpu
from jax.sharding import PartitionSpec as P

MESH = pl.DeviceIdType.MESH
CHIPS = 4
CHUNK = 64
TILES = 4
RING = 16
STAGE = 4
OUT_COPIES = 16
OUT_LIMIT = 1_000_000
SUM_LAG = (0, 2, 5, 3)
DONE_LAG = (24, 6, 24, 24)


def by_place(place, values):
    result = jnp.int32(values[-1])
    for k in range(len(values) - 1):
        result = jnp.where(place == k, jnp.int32(values[k]), result)
    return result


def kernel(
    chunk, tiles, x_hbm, gate_hbm, up_hbm, down_hbm, y_hbm,
    gate_w, up_w, down_w, x_buf, hidden, own, stage, theirs, low, high, sums,
    x_sem, gate_sem, up_sem, down_sem, stage_sem, theirs_sem, low_sem, high_sem,
    sum_sem, spread_sem, pass_sem, y_sem, give_sem, take_sem,
):
    rows, depth = x_hbm.shape
    units = gate_hbm.shape[1]
    half = rows // 2
    chunks = half // chunk
    pieces = chunks * tiles
    unit_tile = units // tiles
    col_tile = depth // tiles

    me = lax.axis_index("tp")
    chip, core = me // 2, me % 2
    place = jnp.where(core == 1, chip, CHIPS - 1 - chip)

    def at_place(k):
        return {"tp": jnp.where(core == 1, k, CHIPS - 1 - k) * 2 + core}

    other = {"tp": me + 1 - 2 * core}
    before, after = at_place(place - 1), at_place(place + 1)
    inner = jnp.logical_or(place == 1, place == 2)

    barrier = pltpu.get_barrier_semaphore()
    pl.semaphore_signal(barrier, inc=1, device_id=other, device_id_type=MESH)

    @pl.when(place > 0)
    def _():
        pl.semaphore_signal(barrier, inc=1, device_id=before, device_id_type=MESH)

    @pl.when(place < CHIPS - 1)
    def _():
        pl.semaphore_signal(barrier, inc=1, device_id=after, device_id_type=MESH)

    def x_rows(which, c):
        return x_hbm.at[pl.ds(pl.multiple_of(which * half + c * chunk, chunk), chunk), :]

    def fetch_x(c):
        slot = lax.rem(c, 2)
        pltpu.make_async_copy(x_rows(core, c), x_buf.at[slot, pl.ds(0, chunk)], x_sem.at[slot]).start()
        pltpu.make_async_copy(x_rows(1 - core, c), x_buf.at[slot, pl.ds(chunk, chunk)], x_sem.at[slot]).start()

    def wait_x(c):
        slot = lax.rem(c, 2)
        pltpu.make_async_copy(x_hbm.at[pl.ds(0, 2 * chunk), :], x_buf.at[slot], x_sem.at[slot]).wait()

    def unit_slice(t):
        return slice(t * unit_tile, (t + 1) * unit_tile)

    def col_slice(t):
        return slice(t * col_tile, (t + 1) * col_tile)

    def gate_copy(t):
        return pltpu.make_async_copy(gate_hbm.at[:, unit_slice(t)], gate_w.at[:, unit_slice(t)], gate_sem.at[t])

    def up_copy(t):
        return pltpu.make_async_copy(up_hbm.at[:, unit_slice(t)], up_w.at[:, unit_slice(t)], up_sem.at[t])

    def down_copy(t):
        return pltpu.make_async_copy(down_hbm.at[:, col_slice(t)], down_w.at[:, col_slice(t)], down_sem.at[t])

    fetch_x(0)
    for t in range(tiles):
        gate_copy(t).start()
        up_copy(t).start()
    def project(c, t):
        slot = lax.rem(c, 2)
        xs = x_buf[slot]
        gate = jnp.dot(xs, gate_w[:, unit_slice(t)], preferred_element_type=jnp.float32)
        up = jnp.dot(xs, up_w[:, unit_slice(t)], preferred_element_type=jnp.float32)
        hidden[slot, :, unit_slice(t)] = (jax.nn.silu(gate) * up).astype(jnp.bfloat16)

    def stage_copy(i):
        slot = lax.rem(i, STAGE)
        return pltpu.make_async_remote_copy(
            src_ref=stage.at[slot], dst_ref=theirs.at[i], send_sem=stage_sem.at[slot], recv_sem=theirs_sem.at[i],
            device_id=other, device_id_type=MESH,
        )

    def terms(c, t):
        i = c * tiles + t
        term = jnp.dot(hidden[lax.rem(c, 2)], down_w[:, col_slice(t)], preferred_element_type=jnp.float32)

        @pl.when(i >= STAGE)
        def _():
            stage_copy(i - STAGE).wait_send()

        stage[lax.rem(i, STAGE)] = term[chunk:].astype(jnp.bfloat16)
        stage_copy(i).start()
        own[lax.rem(i, RING)] = term[:chunk]

    def low_copy(p):
        return pltpu.make_async_remote_copy(
            src_ref=sums.at[p], dst_ref=low.at[p], send_sem=sum_sem, recv_sem=low_sem.at[p],
            device_id=after, device_id_type=MESH,
        )

    def high_copy(p):
        return pltpu.make_async_remote_copy(
            src_ref=sums.at[p], dst_ref=high.at[p], send_sem=sum_sem, recv_sem=high_sem.at[p],
            device_id=before, device_id_type=MESH,
        )

    def spread_copy(p):
        return pltpu.make_async_remote_copy(
            src_ref=sums.at[p], dst_ref=high.at[p], send_sem=spread_sem, recv_sem=high_sem.at[p],
            device_id=after, device_id_type=MESH,
        )

    def pass_copy(p):
        return pltpu.make_async_remote_copy(
            src_ref=high.at[p], dst_ref=high.at[p], send_sem=pass_sem, recv_sem=high_sem.at[p],
            device_id=before, device_id_type=MESH,
        )

    def deliver(src, p):
        c, t = p // tiles, lax.rem(p, tiles)
        block = y_hbm.at[
            pl.ds(pl.multiple_of(core * half + c * chunk, chunk), chunk),
            pl.ds(pl.multiple_of(t * col_tile, col_tile), col_tile),
        ]
        pltpu.make_async_remote_copy(
            src_ref=src, dst_ref=block, send_sem=give_sem, recv_sem=take_sem, device_id=other, device_id_type=MESH,
        ).start()
        pltpu.make_async_copy(src, block, y_sem).start()

    def combine(p):
        pltpu.make_async_copy(theirs.at[p], theirs.at[p], theirs_sem.at[p]).wait()

        def here():
            return own[lax.rem(p, RING)] + theirs[p].astype(jnp.float32)

        @pl.when(jnp.logical_not(inner))
        def _():
            sums[p] = here().astype(jnp.bfloat16)

        @pl.when(inner)
        def _():
            pltpu.make_async_copy(low.at[p], low.at[p], low_sem.at[p]).wait()

        @pl.when(place == 1)
        def _():
            sums[p] = (here() + low[p].astype(jnp.float32)).astype(jnp.bfloat16)

        @pl.when(place == 2)
        def _():
            pltpu.make_async_copy(high.at[p], high.at[p], high_sem.at[p]).wait()
            sums[p] = (here() + low[p].astype(jnp.float32) + high[p].astype(jnp.float32)).astype(jnp.bfloat16)

        @pl.when(place < 2)
        def _():
            low_copy(p).start()

        @pl.when(place >= 2)
        def _():
            high_copy(p).start()

        @pl.when(place == 2)
        def _():
            spread_copy(p).start()
            deliver(sums.at[p], p)

    def finish(p):
        pltpu.make_async_copy(high.at[p], high.at[p], high_sem.at[p]).wait()

        @pl.when(place == 1)
        def _():
            pass_copy(p).start()

        deliver(high.at[p], p)

    sum_lag = by_place(place, SUM_LAG)
    done_lag = by_place(place, DONE_LAG)

    def trail(i):
        p = i - sum_lag

        @pl.when(jnp.logical_and(p >= 0, p < pieces))
        def _():
            combine(p)

        d = i - done_lag

        @pl.when(jnp.logical_and(jnp.logical_and(d >= 0, d < pieces), place != 2))
        def _():
            finish(d)

    wait_x(0)
    for t in range(tiles):
        gate_copy(t).wait()
        up_copy(t).wait()
        if t == tiles // 2:
            for k in range(tiles):
                down_copy(k).start()
            fetch_x(1)
        project(0, t)
    for t in range(tiles):
        down_copy(t).wait()

    pl.semaphore_wait(barrier, jnp.where(inner, 3, 2))

    @pl.loop(0, chunks)
    def _(c):
        @pl.when(c + 2 < chunks)
        def _():
            fetch_x(c + 2)

        @pl.when(c + 1 < chunks)
        def _():
            wait_x(c + 1)

        for t in range(tiles):
            terms(c, t)

            @pl.when(c + 1 < chunks)
            def _():
                project(c + 1, t)

            trail(c * tiles + t)

    @pl.loop(pieces, pieces + max(SUM_LAG + DONE_LAG))
    def _(i):
        trail(i)

    for k in range(STAGE):
        stage_copy(pieces - STAGE + k).wait_send()
    pltpu.make_async_copy(sums, sums, sum_sem).wait()

    @pl.when(place == 2)
    def _():
        pltpu.make_async_copy(sums, sums, spread_sem).wait()

    @pl.when(place == 1)
    def _():
        pltpu.make_async_copy(high, high, pass_sem).wait()

    pltpu.make_async_copy(sums, sums, y_sem).wait()
    pltpu.make_async_copy(sums, sums, give_sem).wait()
    pltpu.make_async_copy(sums, sums, take_sem).wait()


def put_out(y_vmem, y_hbm, sem):
    rows = y_vmem.shape[0] // OUT_COPIES
    for k in range(OUT_COPIES):
        part = pl.ds(k * rows, rows)
        pltpu.make_async_copy(y_vmem.at[part], y_hbm.at[part], sem).start()
    pltpu.make_async_copy(y_vmem, y_hbm, sem).wait()


def block(x, w_gate, w_up, w_down, chunk=CHUNK, tiles=TILES):
    rows, depth = x.shape
    units = w_gate.shape[1]
    pieces = rows // 2 // chunk * tiles
    piece = (chunk, depth // tiles)
    buffers = pltpu.VMEM((pieces,) + piece, jnp.bfloat16)
    dma = pltpu.SemaphoreType.DMA
    anywhere = pl.BlockSpec(memory_space=pl.ANY)
    y = pl.pallas_call(
        functools.partial(kernel, chunk, tiles),
        out_shape=pltpu.VMEM((rows, depth), jnp.bfloat16),
        in_specs=[anywhere] * 4,
        out_specs=anywhere,
        scratch_shapes=[
            pltpu.VMEM((depth, units), jnp.bfloat16),
            pltpu.VMEM((depth, units), jnp.bfloat16),
            pltpu.VMEM((units, depth), jnp.bfloat16),
            pltpu.VMEM((2, 2 * chunk, depth), jnp.bfloat16),
            pltpu.VMEM((2, 2 * chunk, units), jnp.bfloat16),
            pltpu.VMEM((RING,) + piece, jnp.float32),
            pltpu.VMEM((STAGE,) + piece, jnp.bfloat16),
            buffers, buffers, buffers, buffers,
            dma((2,)), dma((tiles,)), dma((tiles,)), dma((tiles,)), dma((STAGE,)),
            dma((pieces,)), dma((pieces,)), dma((pieces,)),
            dma, dma, dma, dma, dma, dma,
        ],
        compiler_params=pltpu.CompilerParams(
            collective_id=0, has_side_effects=True, vmem_limit_bytes=54_000_000
        ),
    )(x, w_gate, w_up, w_down)
    return pl.pallas_call(
        put_out,
        out_shape=jax.ShapeDtypeStruct((rows, depth), jnp.bfloat16),
        in_specs=[anywhere],
        out_specs=anywhere,
        scratch_shapes=[dma],
        compiler_params=pltpu.CompilerParams(vmem_limit_bytes=OUT_LIMIT),
    )(y)


def solution(mesh):
    return jax.shard_map(
        block,
        mesh=mesh,
        in_specs=(P("dp", None), P(None, "tp"), P(None, "tp"), P("tp", None)),
        out_specs=P("dp", None),
        check_vma=False,
    )
```

```python
import functools

import jax
import jax.numpy as jnp
from jax import lax
from jax.experimental import pallas as pl
from jax.experimental.pallas import tpu as pltpu
from jax.sharding import PartitionSpec as P

MESH = pl.DeviceIdType.MESH
CHIPS = 4
CHUNK = 64
TILES = 4
RING = 16
STAGE = 4
OUT_COPIES = 16
OUT_LIMIT = 1_000_000
SUM_LAG = (0, 2, 5, 3)
DONE_LAG = (24, 6, 24, 24)


def by_place(place, values):
    result = jnp.int32(values[-1])
    for k in range(len(values) - 1):
        result = jnp.where(place == k, jnp.int32(values[k]), result)
    return result


def kernel(
    chunk, tiles, x_hbm, gate_hbm, up_hbm, down_hbm, y_hbm,
    gate_w, up_w, down_w, x_buf, hidden, first_gate, first_up, own, stage, theirs, low, high, sums,
    x_sem, gate_sem, up_sem, down_sem, stage_sem, theirs_sem, low_sem, high_sem,
    sum_sem, spread_sem, pass_sem, y_sem, give_sem, take_sem,
):
    rows, depth = x_hbm.shape
    units = gate_hbm.shape[1]
    half = rows // 2
    chunks = half // chunk
    pieces = chunks * tiles
    unit_tile = units // tiles
    col_tile = depth // tiles

    me = lax.axis_index("tp")
    chip, core = me // 2, me % 2
    place = jnp.where(core == 1, chip, CHIPS - 1 - chip)

    def at_place(k):
        return {"tp": jnp.where(core == 1, k, CHIPS - 1 - k) * 2 + core}

    other = {"tp": me + 1 - 2 * core}
    before, after = at_place(place - 1), at_place(place + 1)
    inner = jnp.logical_or(place == 1, place == 2)

    barrier = pltpu.get_barrier_semaphore()
    pl.semaphore_signal(barrier, inc=1, device_id=other, device_id_type=MESH)

    @pl.when(place > 0)
    def _():
        pl.semaphore_signal(barrier, inc=1, device_id=before, device_id_type=MESH)

    @pl.when(place < CHIPS - 1)
    def _():
        pl.semaphore_signal(barrier, inc=1, device_id=after, device_id_type=MESH)

    def x_rows(which, c):
        return x_hbm.at[pl.ds(pl.multiple_of(which * half + c * chunk, chunk), chunk), :]

    def fetch_x(c):
        slot = lax.rem(c, 2)
        pltpu.make_async_copy(x_rows(core, c), x_buf.at[slot, pl.ds(0, chunk)], x_sem.at[slot]).start()
        pltpu.make_async_copy(x_rows(1 - core, c), x_buf.at[slot, pl.ds(chunk, chunk)], x_sem.at[slot]).start()

    def wait_x(c):
        slot = lax.rem(c, 2)
        pltpu.make_async_copy(x_hbm.at[pl.ds(0, 2 * chunk), :], x_buf.at[slot], x_sem.at[slot]).wait()

    depth_tile = depth // tiles

    def unit_slice(t):
        return pl.ds(pl.multiple_of(t * unit_tile, unit_tile), unit_tile)

    def depth_slice(k):
        return pl.ds(pl.multiple_of(k * depth_tile, depth_tile), depth_tile)

    def col_slice(t):
        return pl.ds(pl.multiple_of(t * col_tile, col_tile), col_tile)

    def gate_copy(k):
        return pltpu.make_async_copy(gate_hbm.at[depth_slice(k)], gate_w.at[depth_slice(k)], gate_sem.at[k])

    def up_copy(k):
        return pltpu.make_async_copy(up_hbm.at[depth_slice(k)], up_w.at[depth_slice(k)], up_sem.at[k])

    def down_copy(t):
        return pltpu.make_async_copy(down_hbm.at[:, col_slice(t)], down_w.at[:, col_slice(t)], down_sem.at[t])

    def dot(a, b):
        return jnp.dot(a, b, preferred_element_type=jnp.float32)

    def activate(gate, up):
        return (jax.nn.silu(gate) * up).astype(jnp.bfloat16)

    def project(c, t):
        slot = lax.rem(c, 2)
        xs = x_buf[slot]
        hidden[slot, :, unit_slice(t)] = activate(dot(xs, gate_w[:, unit_slice(t)]), dot(xs, up_w[:, unit_slice(t)]))

    fetch_x(0)
    for k in range(tiles):
        gate_copy(k).start()
        up_copy(k).start()

    def stage_copy(i):
        slot = lax.rem(i, STAGE)
        return pltpu.make_async_remote_copy(
            src_ref=stage.at[slot], dst_ref=theirs.at[i], send_sem=stage_sem.at[slot], recv_sem=theirs_sem.at[i],
            device_id=other, device_id_type=MESH,
        )

    def terms(c, t):
        i = c * tiles + t
        term = dot(hidden[lax.rem(c, 2)], down_w[:, col_slice(t)])

        @pl.when(i >= STAGE)
        def _():
            stage_copy(i - STAGE).wait_send()

        stage[lax.rem(i, STAGE)] = term[chunk:].astype(jnp.bfloat16)
        stage_copy(i).start()
        own[lax.rem(i, RING)] = term[:chunk]

    def low_copy(p):
        return pltpu.make_async_remote_copy(
            src_ref=sums.at[p], dst_ref=low.at[p], send_sem=sum_sem, recv_sem=low_sem.at[p],
            device_id=after, device_id_type=MESH,
        )

    def high_copy(p):
        return pltpu.make_async_remote_copy(
            src_ref=sums.at[p], dst_ref=high.at[p], send_sem=sum_sem, recv_sem=high_sem.at[p],
            device_id=before, device_id_type=MESH,
        )

    def spread_copy(p):
        return pltpu.make_async_remote_copy(
            src_ref=sums.at[p], dst_ref=high.at[p], send_sem=spread_sem, recv_sem=high_sem.at[p],
            device_id=after, device_id_type=MESH,
        )

    def pass_copy(p):
        return pltpu.make_async_remote_copy(
            src_ref=high.at[p], dst_ref=high.at[p], send_sem=pass_sem, recv_sem=high_sem.at[p],
            device_id=before, device_id_type=MESH,
        )

    def deliver(src, p):
        c, t = p // tiles, lax.rem(p, tiles)
        block = y_hbm.at[
            pl.ds(pl.multiple_of(core * half + c * chunk, chunk), chunk),
            pl.ds(pl.multiple_of(t * col_tile, col_tile), col_tile),
        ]
        pltpu.make_async_remote_copy(
            src_ref=src, dst_ref=block, send_sem=give_sem, recv_sem=take_sem, device_id=other, device_id_type=MESH,
        ).start()
        pltpu.make_async_copy(src, block, y_sem).start()

    def combine(p):
        pltpu.make_async_copy(theirs.at[p], theirs.at[p], theirs_sem.at[p]).wait()

        def here():
            return own[lax.rem(p, RING)] + theirs[p].astype(jnp.float32)

        @pl.when(jnp.logical_not(inner))
        def _():
            sums[p] = here().astype(jnp.bfloat16)

        @pl.when(inner)
        def _():
            pltpu.make_async_copy(low.at[p], low.at[p], low_sem.at[p]).wait()

        @pl.when(place == 1)
        def _():
            sums[p] = (here() + low[p].astype(jnp.float32)).astype(jnp.bfloat16)

        @pl.when(place == 2)
        def _():
            pltpu.make_async_copy(high.at[p], high.at[p], high_sem.at[p]).wait()
            sums[p] = (here() + low[p].astype(jnp.float32) + high[p].astype(jnp.float32)).astype(jnp.bfloat16)

        @pl.when(place < 2)
        def _():
            low_copy(p).start()

        @pl.when(place >= 2)
        def _():
            high_copy(p).start()

        @pl.when(place == 2)
        def _():
            spread_copy(p).start()
            deliver(sums.at[p], p)

    def finish(p):
        pltpu.make_async_copy(high.at[p], high.at[p], high_sem.at[p]).wait()

        @pl.when(place == 1)
        def _():
            pass_copy(p).start()

        deliver(high.at[p], p)

    sum_lag = by_place(place, SUM_LAG)
    done_lag = by_place(place, DONE_LAG)

    def trail(i):
        p = i - sum_lag

        @pl.when(jnp.logical_and(p >= 0, p < pieces))
        def _():
            combine(p)

        d = i - done_lag

        @pl.when(jnp.logical_and(jnp.logical_and(d >= 0, d < pieces), place != 2))
        def _():
            finish(d)

    wait_x(0)

    @pl.loop(0, tiles)
    def _(k):
        gate_copy(k).wait()
        up_copy(k).wait()

        @pl.when(k == tiles // 2)
        def _():
            for t in range(tiles):
                down_copy(t).start()
            fetch_x(1)

        xs = x_buf[0, :, depth_slice(k)]
        gate = dot(xs, gate_w[depth_slice(k)])
        up = dot(xs, up_w[depth_slice(k)])

        @pl.when(k == 0)
        def _():
            first_gate[...] = gate
            first_up[...] = up

        @pl.when(k > 0)
        def _():
            first_gate[...] += gate
            first_up[...] += up

    hidden[0] = activate(first_gate[...], first_up[...])
    pl.semaphore_wait(barrier, jnp.where(inner, 3, 2))

    @pl.loop(0, pieces + max(SUM_LAG + DONE_LAG))
    def _(i):
        c, t = i // tiles, lax.rem(i, tiles)

        @pl.when(i < pieces)
        def _():
            @pl.when(c == 0)
            def _():
                down_copy(t).wait()

            @pl.when(jnp.logical_and(t == 0, c + 2 < chunks))
            def _():
                fetch_x(c + 2)

            @pl.when(jnp.logical_and(t == 0, c + 1 < chunks))
            def _():
                wait_x(c + 1)

            terms(c, t)

            @pl.when(c + 1 < chunks)
            def _():
                project(c + 1, t)

        trail(i)

    for k in range(STAGE):
        stage_copy(pieces - STAGE + k).wait_send()
    pltpu.make_async_copy(sums, sums, sum_sem).wait()

    @pl.when(place == 2)
    def _():
        pltpu.make_async_copy(sums, sums, spread_sem).wait()

    @pl.when(place == 1)
    def _():
        pltpu.make_async_copy(high, high, pass_sem).wait()

    pltpu.make_async_copy(sums, sums, y_sem).wait()
    pltpu.make_async_copy(sums, sums, give_sem).wait()
    pltpu.make_async_copy(sums, sums, take_sem).wait()


def put_out(y_vmem, y_hbm, sem):
    rows = y_vmem.shape[0] // OUT_COPIES
    for k in range(OUT_COPIES):
        part = pl.ds(k * rows, rows)
        pltpu.make_async_copy(y_vmem.at[part], y_hbm.at[part], sem).start()
    pltpu.make_async_copy(y_vmem, y_hbm, sem).wait()


def block(x, w_gate, w_up, w_down, chunk=CHUNK, tiles=TILES):
    rows, depth = x.shape
    units = w_gate.shape[1]
    pieces = rows // 2 // chunk * tiles
    piece = (chunk, depth // tiles)
    buffers = pltpu.VMEM((pieces,) + piece, jnp.bfloat16)
    dma = pltpu.SemaphoreType.DMA
    anywhere = pl.BlockSpec(memory_space=pl.ANY)
    y = pl.pallas_call(
        functools.partial(kernel, chunk, tiles),
        out_shape=pltpu.VMEM((rows, depth), jnp.bfloat16),
        in_specs=[anywhere] * 4,
        out_specs=anywhere,
        scratch_shapes=[
            pltpu.VMEM((depth, units), jnp.bfloat16),
            pltpu.VMEM((depth, units), jnp.bfloat16),
            pltpu.VMEM((units, depth), jnp.bfloat16),
            pltpu.VMEM((2, 2 * chunk, depth), jnp.bfloat16),
            pltpu.VMEM((2, 2 * chunk, units), jnp.bfloat16),
            pltpu.VMEM((2 * chunk, units), jnp.float32),
            pltpu.VMEM((2 * chunk, units), jnp.float32),
            pltpu.VMEM((RING,) + piece, jnp.float32),
            pltpu.VMEM((STAGE,) + piece, jnp.bfloat16),
            buffers, buffers, buffers, buffers,
            dma((2,)), dma((tiles,)), dma((tiles,)), dma((tiles,)), dma((STAGE,)),
            dma((pieces,)), dma((pieces,)), dma((pieces,)),
            dma, dma, dma, dma, dma, dma,
        ],
        compiler_params=pltpu.CompilerParams(
            collective_id=0, has_side_effects=True, vmem_limit_bytes=54_000_000
        ),
    )(x, w_gate, w_up, w_down)
    return pl.pallas_call(
        put_out,
        out_shape=jax.ShapeDtypeStruct((rows, depth), jnp.bfloat16),
        in_specs=[anywhere],
        out_specs=anywhere,
        scratch_shapes=[dma],
        compiler_params=pltpu.CompilerParams(vmem_limit_bytes=OUT_LIMIT),
    )(y)


def solution(mesh):
    return jax.shard_map(
        block,
        mesh=mesh,
        in_specs=(P("dp", None), P(None, "tp"), P(None, "tp"), P("tp", None)),
        out_specs=P("dp", None),
        check_vma=False,
    )
```

```python
import functools

import jax
import jax.numpy as jnp
from jax import lax
from jax.experimental import pallas as pl
from jax.experimental.pallas import tpu as pltpu
from jax.sharding import PartitionSpec as P

MESH = pl.DeviceIdType.MESH
CHIPS = 4
CHUNK = 64
TILES = 4
RING = 16
STAGE = 4
OUT_COPIES = 16
OUT_LIMIT = 1_000_000
SUM_LAG = ((0, 2, 4, 3), (0, 2, 4, 5))
DONE_LAG = ((24, 7, 24, 24), (24, 6, 24, 24))
PARTS = 2
HEAD = 8
AHEAD = 4


def by_place(core, place, rows):
    result = jnp.int32(rows[-1][-1])
    for k, row in enumerate(rows):
        for j, value in enumerate(row):
            result = jnp.where(jnp.logical_and(core == k, place == j), jnp.int32(value), result)
    return result


LONGEST = max(max(row) for row in SUM_LAG + DONE_LAG)


def kernel(
    chunk, tiles, x_hbm, gate_hbm, up_hbm, down_hbm, y_hbm,
    gate_w, up_w, down_w, x_buf, hidden, first_gate, first_up, own, stage, theirs, low, high, sums,
    x_sem, gate_sem, up_sem, down_sem, stage_sem, theirs_sem, low_sem, high_sem,
    sum_sem, spread_sem, pass_sem, y_sem, give_sem, take_sem,
):
    rows, depth = x_hbm.shape
    units = gate_hbm.shape[1]
    half = rows // 2
    chunks = half // chunk
    pieces = chunks * tiles
    unit_tile = units // tiles
    col_tile = depth // tiles

    me = lax.axis_index("tp")
    chip, core = me // 2, me % 2
    place = jnp.where(core == 1, chip, CHIPS - 1 - chip)

    def at_place(k):
        return {"tp": jnp.where(core == 1, k, CHIPS - 1 - k) * 2 + core}

    other = {"tp": me + 1 - 2 * core}
    before, after = at_place(place - 1), at_place(place + 1)
    inner = jnp.logical_or(place == 1, place == 2)

    barrier = pltpu.get_barrier_semaphore()
    pl.semaphore_signal(barrier, inc=1, device_id=other, device_id_type=MESH)

    @pl.when(place > 0)
    def _():
        pl.semaphore_signal(barrier, inc=1, device_id=before, device_id_type=MESH)

    @pl.when(place < CHIPS - 1)
    def _():
        pl.semaphore_signal(barrier, inc=1, device_id=after, device_id_type=MESH)

    def x_rows(which, c):
        return x_hbm.at[pl.ds(pl.multiple_of(which * half + c * chunk, chunk), chunk), :]

    def fetch_x(c):
        slot = lax.rem(c, 2)
        pltpu.make_async_copy(x_rows(core, c), x_buf.at[slot, pl.ds(0, chunk)], x_sem.at[slot]).start()
        pltpu.make_async_copy(x_rows(1 - core, c), x_buf.at[slot, pl.ds(chunk, chunk)], x_sem.at[slot]).start()

    def wait_x(c):
        slot = lax.rem(c, 2)
        pltpu.make_async_copy(x_hbm.at[pl.ds(0, 2 * chunk), :], x_buf.at[slot], x_sem.at[slot]).wait()

    depth_tile = depth // HEAD
    part_tile = col_tile // PARTS

    def unit_slice(t):
        return pl.ds(pl.multiple_of(t * unit_tile, unit_tile), unit_tile)

    def depth_slice(k):
        return pl.ds(pl.multiple_of(k * depth_tile, depth_tile), depth_tile)

    def col_slice(t):
        return pl.ds(pl.multiple_of(t * col_tile, col_tile), col_tile)

    def gate_copy(k):
        return pltpu.make_async_copy(gate_hbm.at[depth_slice(k)], gate_w.at[depth_slice(k)], gate_sem.at[k])

    def up_copy(k):
        return pltpu.make_async_copy(up_hbm.at[depth_slice(k)], up_w.at[depth_slice(k)], up_sem.at[k])

    def down_copy(t):
        return pltpu.make_async_copy(down_hbm.at[:, col_slice(t)], down_w.at[:, col_slice(t)], down_sem.at[t])

    def dot(a, b):
        return jnp.dot(a, b, preferred_element_type=jnp.float32)

    def activate(gate, up):
        return (jax.nn.silu(gate) * up).astype(jnp.bfloat16)

    def project(c, t):
        slot = lax.rem(c, 2)
        xs = x_buf[slot]
        hidden[slot, :, unit_slice(t)] = activate(dot(xs, gate_w[:, unit_slice(t)]), dot(xs, up_w[:, unit_slice(t)]))

    fetch_x(0)
    for k in range(AHEAD):
        gate_copy(k).start()
        up_copy(k).start()

    def stage_copy(i):
        slot = lax.rem(i, STAGE)
        return pltpu.make_async_remote_copy(
            src_ref=stage.at[slot], dst_ref=theirs.at[i], send_sem=stage_sem.at[slot], recv_sem=theirs_sem.at[i],
            device_id=other, device_id_type=MESH,
        )

    def terms(c, t):
        i = c * tiles + t
        term = dot(hidden[lax.rem(c, 2)], down_w[:, col_slice(t)])

        @pl.when(i >= STAGE)
        def _():
            stage_copy(i - STAGE).wait_send()

        stage[lax.rem(i, STAGE)] = term[chunk:].astype(jnp.bfloat16)
        stage_copy(i).start()
        own[lax.rem(i, RING)] = term[:chunk]

    def low_copy(p):
        return pltpu.make_async_remote_copy(
            src_ref=sums.at[p], dst_ref=low.at[p], send_sem=sum_sem, recv_sem=low_sem.at[p],
            device_id=after, device_id_type=MESH,
        )

    def high_copy(p):
        return pltpu.make_async_remote_copy(
            src_ref=sums.at[p], dst_ref=high.at[p], send_sem=sum_sem, recv_sem=high_sem.at[p],
            device_id=before, device_id_type=MESH,
        )

    def spread_copy(p):
        return pltpu.make_async_remote_copy(
            src_ref=sums.at[p], dst_ref=high.at[p], send_sem=spread_sem, recv_sem=high_sem.at[p],
            device_id=after, device_id_type=MESH,
        )

    def pass_copy(p):
        return pltpu.make_async_remote_copy(
            src_ref=high.at[p], dst_ref=high.at[p], send_sem=pass_sem, recv_sem=high_sem.at[p],
            device_id=before, device_id_type=MESH,
        )

    def deliver(src, m):
        p = m // PARTS
        c, column = p // tiles, lax.rem(p, tiles) * col_tile + lax.rem(m, PARTS) * part_tile
        block = y_hbm.at[
            pl.ds(pl.multiple_of(core * half + c * chunk, chunk), chunk),
            pl.ds(pl.multiple_of(column, part_tile), part_tile),
        ]
        pltpu.make_async_remote_copy(
            src_ref=src, dst_ref=block, send_sem=give_sem, recv_sem=take_sem, device_id=other, device_id_type=MESH,
        ).start()
        pltpu.make_async_copy(src, block, y_sem).start()

    def combine(p):
        pltpu.make_async_copy(theirs.at[p], theirs.at[p], theirs_sem.at[p]).wait()
        for part in range(PARTS):
            combine_part(p, part)

    def combine_part(p, part):
        m = p * PARTS + part
        columns = slice(part * part_tile, (part + 1) * part_tile)

        def here():
            return own[lax.rem(p, RING), :, columns] + theirs[p, :, columns].astype(jnp.float32)

        @pl.when(jnp.logical_not(inner))
        def _():
            sums[m] = here().astype(jnp.bfloat16)

        @pl.when(inner)
        def _():
            pltpu.make_async_copy(low.at[m], low.at[m], low_sem.at[m]).wait()

        @pl.when(place == 1)
        def _():
            sums[m] = (here() + low[m].astype(jnp.float32)).astype(jnp.bfloat16)

        @pl.when(place == 2)
        def _():
            pltpu.make_async_copy(high.at[m], high.at[m], high_sem.at[m]).wait()
            sums[m] = (here() + low[m].astype(jnp.float32) + high[m].astype(jnp.float32)).astype(jnp.bfloat16)

        @pl.when(place < 2)
        def _():
            low_copy(m).start()

        @pl.when(place >= 2)
        def _():
            high_copy(m).start()

        @pl.when(place == 2)
        def _():
            spread_copy(m).start()
            deliver(sums.at[m], m)

    def finish(p):
        for part in range(PARTS):
            m = p * PARTS + part
            pltpu.make_async_copy(high.at[m], high.at[m], high_sem.at[m]).wait()

            @pl.when(place == 1)
            def _():
                pass_copy(m).start()

            deliver(high.at[m], m)

    sum_lag = by_place(core, place, SUM_LAG)
    done_lag = by_place(core, place, DONE_LAG)

    def trail(i):
        p = i - sum_lag

        @pl.when(jnp.logical_and(p >= 0, p < pieces))
        def _():
            combine(p)

        d = i - done_lag

        @pl.when(jnp.logical_and(jnp.logical_and(d >= 0, d < pieces), place != 2))
        def _():
            finish(d)

    wait_x(0)

    @pl.loop(0, HEAD)
    def _(k):
        gate_copy(k).wait()
        up_copy(k).wait()

        @pl.when(k + AHEAD < HEAD)
        def _():
            gate_copy(k + AHEAD).start()
            up_copy(k + AHEAD).start()

        @pl.when(k + AHEAD >= HEAD)
        def _():
            down_copy(k + AHEAD - HEAD).start()

        @pl.when(k == HEAD - 1)
        def _():
            fetch_x(1)

        xs = x_buf[0, :, depth_slice(k)]
        gate = dot(xs, gate_w[depth_slice(k)])
        up = dot(xs, up_w[depth_slice(k)])

        @pl.when(k == 0)
        def _():
            first_gate[...] = gate
            first_up[...] = up

        @pl.when(k > 0)
        def _():
            first_gate[...] += gate
            first_up[...] += up

    hidden[0] = activate(first_gate[...], first_up[...])
    pl.semaphore_wait(barrier, jnp.where(inner, 3, 2))

    @pl.loop(0, pieces + LONGEST)
    def _(i):
        c, t = i // tiles, lax.rem(i, tiles)

        @pl.when(i < pieces)
        def _():
            @pl.when(c == 0)
            def _():
                down_copy(t).wait()

            @pl.when(jnp.logical_and(t == 0, c + 2 < chunks))
            def _():
                fetch_x(c + 2)

            @pl.when(jnp.logical_and(t == 0, c + 1 < chunks))
            def _():
                wait_x(c + 1)

            terms(c, t)

            @pl.when(c + 1 < chunks)
            def _():
                project(c + 1, t)

        trail(i)

    for k in range(STAGE):
        stage_copy(pieces - STAGE + k).wait_send()
    pltpu.make_async_copy(sums, sums, sum_sem).wait()

    @pl.when(place == 2)
    def _():
        pltpu.make_async_copy(sums, sums, spread_sem).wait()

    @pl.when(place == 1)
    def _():
        pltpu.make_async_copy(high, high, pass_sem).wait()

    pltpu.make_async_copy(sums, sums, y_sem).wait()
    pltpu.make_async_copy(sums, sums, give_sem).wait()
    pltpu.make_async_copy(sums, sums, take_sem).wait()


def put_out(y_vmem, y_hbm, sem):
    rows = y_vmem.shape[0] // OUT_COPIES
    for k in range(OUT_COPIES):
        part = pl.ds(k * rows, rows)
        pltpu.make_async_copy(y_vmem.at[part], y_hbm.at[part], sem).start()
    pltpu.make_async_copy(y_vmem, y_hbm, sem).wait()


def block(x, w_gate, w_up, w_down, chunk=CHUNK, tiles=TILES):
    rows, depth = x.shape
    units = w_gate.shape[1]
    pieces = rows // 2 // chunk * tiles
    piece = (chunk, depth // tiles)
    messages = pieces * PARTS
    buffers = pltpu.VMEM((messages, chunk, depth // tiles // PARTS), jnp.bfloat16)
    dma = pltpu.SemaphoreType.DMA
    anywhere = pl.BlockSpec(memory_space=pl.ANY)
    y = pl.pallas_call(
        functools.partial(kernel, chunk, tiles),
        out_shape=pltpu.VMEM((rows, depth), jnp.bfloat16),
        in_specs=[anywhere] * 4,
        out_specs=anywhere,
        scratch_shapes=[
            pltpu.VMEM((depth, units), jnp.bfloat16),
            pltpu.VMEM((depth, units), jnp.bfloat16),
            pltpu.VMEM((units, depth), jnp.bfloat16),
            pltpu.VMEM((2, 2 * chunk, depth), jnp.bfloat16),
            pltpu.VMEM((2, 2 * chunk, units), jnp.bfloat16),
            pltpu.VMEM((2 * chunk, units), jnp.float32),
            pltpu.VMEM((2 * chunk, units), jnp.float32),
            pltpu.VMEM((RING,) + piece, jnp.float32),
            pltpu.VMEM((STAGE,) + piece, jnp.bfloat16),
            pltpu.VMEM((pieces,) + piece, jnp.bfloat16), buffers, buffers, buffers,
            dma((2,)), dma((HEAD,)), dma((HEAD,)), dma((tiles,)), dma((STAGE,)),
            dma((pieces,)), dma((messages,)), dma((messages,)),
            dma, dma, dma, dma, dma, dma,
        ],
        compiler_params=pltpu.CompilerParams(
            collective_id=0, has_side_effects=True, vmem_limit_bytes=54_000_000
        ),
    )(x, w_gate, w_up, w_down)
    return pl.pallas_call(
        put_out,
        out_shape=jax.ShapeDtypeStruct((rows, depth), jnp.bfloat16),
        in_specs=[anywhere],
        out_specs=anywhere,
        scratch_shapes=[dma],
        compiler_params=pltpu.CompilerParams(vmem_limit_bytes=OUT_LIMIT),
    )(y)


def solution(mesh):
    return jax.shard_map(
        block,
        mesh=mesh,
        in_specs=(P("dp", None), P(None, "tp"), P(None, "tp"), P("tp", None)),
        out_specs=P("dp", None),
        check_vma=False,
    )
```

```python
import functools

import jax
import jax.numpy as jnp
from jax import lax
from jax.experimental import pallas as pl
from jax.experimental.pallas import tpu as pltpu
from jax.sharding import PartitionSpec as P

MESH = pl.DeviceIdType.MESH
CHIPS = 4
CHUNK = 64
TILES = 4
RING = 16
STAGE = 4
OUT_COPIES = 16
OUT_LIMIT = 1_000_000
SUM_LAG = ((0, 2, 5, 4), (0, 2, 5, 4))
DONE_LAG = ((24, 6, 24, 24), (24, 6, 24, 24))
PARTS = 1
HEAD = 6
AHEAD = 5
DOWN_AT = 2


def by_place(core, place, rows):
    result = jnp.int32(rows[-1][-1])
    for k, row in enumerate(rows):
        for j, value in enumerate(row):
            result = jnp.where(jnp.logical_and(core == k, place == j), jnp.int32(value), result)
    return result


LONGEST = max(max(row) for row in SUM_LAG + DONE_LAG)


def kernel(
    chunk, tiles, x_hbm, gate_hbm, up_hbm, down_hbm, y_hbm,
    gate_w, up_w, down_w, x_buf, hidden, first_gate, first_up, own, stage, theirs, low, high, sums,
    x_sem, gate_sem, up_sem, down_sem, stage_sem, theirs_sem, low_sem, high_sem,
    sum_sem, spread_sem, pass_sem, y_sem, give_sem, take_sem,
):
    rows, depth = x_hbm.shape
    units = gate_hbm.shape[1]
    half = rows // 2
    chunks = half // chunk
    pieces = chunks * tiles
    unit_tile = units // tiles
    col_tile = depth // tiles

    me = lax.axis_index("tp")
    chip, core = me // 2, me % 2
    place = jnp.where(core == 1, chip, CHIPS - 1 - chip)

    def at_place(k):
        return {"tp": jnp.where(core == 1, k, CHIPS - 1 - k) * 2 + core}

    other = {"tp": me + 1 - 2 * core}
    before, after = at_place(place - 1), at_place(place + 1)
    inner = jnp.logical_or(place == 1, place == 2)

    barrier = pltpu.get_barrier_semaphore()
    pl.semaphore_signal(barrier, inc=1, device_id=other, device_id_type=MESH)

    @pl.when(place > 0)
    def _():
        pl.semaphore_signal(barrier, inc=1, device_id=before, device_id_type=MESH)

    @pl.when(place < CHIPS - 1)
    def _():
        pl.semaphore_signal(barrier, inc=1, device_id=after, device_id_type=MESH)

    def x_rows(which, c):
        return x_hbm.at[pl.ds(pl.multiple_of(which * half + c * chunk, chunk), chunk), :]

    def fetch_x(c):
        slot = lax.rem(c, 2)
        pltpu.make_async_copy(x_rows(core, c), x_buf.at[slot, pl.ds(0, chunk)], x_sem.at[slot]).start()
        pltpu.make_async_copy(x_rows(1 - core, c), x_buf.at[slot, pl.ds(chunk, chunk)], x_sem.at[slot]).start()

    def wait_x(c):
        slot = lax.rem(c, 2)
        pltpu.make_async_copy(x_hbm.at[pl.ds(0, 2 * chunk), :], x_buf.at[slot], x_sem.at[slot]).wait()

    depth_tile = depth // HEAD
    part_tile = col_tile // PARTS

    def unit_slice(t):
        return pl.ds(pl.multiple_of(t * unit_tile, unit_tile), unit_tile)

    def depth_slice(k):
        return pl.ds(pl.multiple_of(k * depth_tile, depth_tile), depth_tile)

    def col_slice(t):
        return pl.ds(pl.multiple_of(t * col_tile, col_tile), col_tile)

    def gate_copy(k):
        return pltpu.make_async_copy(gate_hbm.at[depth_slice(k)], gate_w.at[depth_slice(k)], gate_sem.at[k])

    def up_copy(k):
        return pltpu.make_async_copy(up_hbm.at[depth_slice(k)], up_w.at[depth_slice(k)], up_sem.at[k])

    def down_copy(t):
        return pltpu.make_async_copy(down_hbm.at[:, col_slice(t)], down_w.at[:, col_slice(t)], down_sem.at[t])

    def dot(a, b):
        return jnp.dot(a, b, preferred_element_type=jnp.float32)

    def activate(gate, up):
        return (jax.nn.silu(gate) * up).astype(jnp.bfloat16)

    def project(c, t):
        slot = lax.rem(c, 2)
        xs = x_buf[slot]
        hidden[slot, :, unit_slice(t)] = activate(dot(xs, gate_w[:, unit_slice(t)]), dot(xs, up_w[:, unit_slice(t)]))

    fetch_x(0)
    for k in range(AHEAD):
        gate_copy(k).start()
        up_copy(k).start()

    def stage_copy(i):
        slot = lax.rem(i, STAGE)
        return pltpu.make_async_remote_copy(
            src_ref=stage.at[slot], dst_ref=theirs.at[i], send_sem=stage_sem.at[slot], recv_sem=theirs_sem.at[i],
            device_id=other, device_id_type=MESH,
        )

    def terms(c, t):
        i = c * tiles + t
        term = dot(hidden[lax.rem(c, 2)], down_w[:, col_slice(t)])

        @pl.when(i >= STAGE)
        def _():
            stage_copy(i - STAGE).wait_send()

        stage[lax.rem(i, STAGE)] = term[chunk:].astype(jnp.bfloat16)
        stage_copy(i).start()
        own[lax.rem(i, RING)] = term[:chunk]

    def low_copy(p):
        return pltpu.make_async_remote_copy(
            src_ref=sums.at[p], dst_ref=low.at[p], send_sem=sum_sem, recv_sem=low_sem.at[p],
            device_id=after, device_id_type=MESH,
        )

    def high_copy(p):
        return pltpu.make_async_remote_copy(
            src_ref=sums.at[p], dst_ref=high.at[p], send_sem=sum_sem, recv_sem=high_sem.at[p],
            device_id=before, device_id_type=MESH,
        )

    def spread_copy(p):
        return pltpu.make_async_remote_copy(
            src_ref=sums.at[p], dst_ref=high.at[p], send_sem=spread_sem, recv_sem=high_sem.at[p],
            device_id=after, device_id_type=MESH,
        )

    def pass_copy(p):
        return pltpu.make_async_remote_copy(
            src_ref=high.at[p], dst_ref=high.at[p], send_sem=pass_sem, recv_sem=high_sem.at[p],
            device_id=before, device_id_type=MESH,
        )

    def deliver(src, m):
        p = m // PARTS
        c, column = p // tiles, lax.rem(p, tiles) * col_tile + lax.rem(m, PARTS) * part_tile
        block = y_hbm.at[
            pl.ds(pl.multiple_of(core * half + c * chunk, chunk), chunk),
            pl.ds(pl.multiple_of(column, part_tile), part_tile),
        ]
        pltpu.make_async_remote_copy(
            src_ref=src, dst_ref=block, send_sem=give_sem, recv_sem=take_sem, device_id=other, device_id_type=MESH,
        ).start()
        pltpu.make_async_copy(src, block, y_sem).start()

    def combine(p):
        pltpu.make_async_copy(theirs.at[p], theirs.at[p], theirs_sem.at[p]).wait()
        for part in range(PARTS):
            combine_part(p, part)

    def combine_part(p, part):
        m = p * PARTS + part
        columns = slice(part * part_tile, (part + 1) * part_tile)

        def here():
            return own[lax.rem(p, RING), :, columns] + theirs[p, :, columns].astype(jnp.float32)

        @pl.when(jnp.logical_not(inner))
        def _():
            sums[m] = here().astype(jnp.bfloat16)

        @pl.when(inner)
        def _():
            pltpu.make_async_copy(low.at[m], low.at[m], low_sem.at[m]).wait()

        @pl.when(place == 1)
        def _():
            sums[m] = (here() + low[m].astype(jnp.float32)).astype(jnp.bfloat16)

        @pl.when(place == 2)
        def _():
            pltpu.make_async_copy(high.at[m], high.at[m], high_sem.at[m]).wait()
            sums[m] = (here() + low[m].astype(jnp.float32) + high[m].astype(jnp.float32)).astype(jnp.bfloat16)

        @pl.when(place < 2)
        def _():
            low_copy(m).start()

        @pl.when(place >= 2)
        def _():
            high_copy(m).start()

        @pl.when(place == 2)
        def _():
            spread_copy(m).start()
            deliver(sums.at[m], m)

    def finish(p):
        for part in range(PARTS):
            m = p * PARTS + part
            pltpu.make_async_copy(high.at[m], high.at[m], high_sem.at[m]).wait()

            @pl.when(place == 1)
            def _():
                pass_copy(m).start()

            deliver(high.at[m], m)

    sum_lag = by_place(core, place, SUM_LAG)
    done_lag = by_place(core, place, DONE_LAG)

    def trail(i):
        p = i - sum_lag

        @pl.when(jnp.logical_and(p >= 0, p < pieces))
        def _():
            combine(p)

        d = i - done_lag

        @pl.when(jnp.logical_and(jnp.logical_and(d >= 0, d < pieces), place != 2))
        def _():
            finish(d)

    wait_x(0)

    @pl.loop(0, HEAD)
    def _(k):
        gate_copy(k).wait()
        up_copy(k).wait()

        @pl.when(k + AHEAD < HEAD)
        def _():
            gate_copy(k + AHEAD).start()
            up_copy(k + AHEAD).start()

        @pl.when(k == DOWN_AT)
        def _():
            for t in range(tiles):
                down_copy(t).start()
            fetch_x(1)

        xs = x_buf[0, :, depth_slice(k)]
        gate = dot(xs, gate_w[depth_slice(k)])
        up = dot(xs, up_w[depth_slice(k)])

        @pl.when(k == 0)
        def _():
            first_gate[...] = gate
            first_up[...] = up

        @pl.when(k > 0)
        def _():
            first_gate[...] += gate
            first_up[...] += up

    hidden[0] = activate(first_gate[...], first_up[...])
    pl.semaphore_wait(barrier, jnp.where(inner, 3, 2))

    @pl.loop(0, pieces + LONGEST)
    def _(i):
        c, t = i // tiles, lax.rem(i, tiles)

        @pl.when(i < pieces)
        def _():
            @pl.when(c == 0)
            def _():
                down_copy(t).wait()

            @pl.when(jnp.logical_and(t == 0, c + 2 < chunks))
            def _():
                fetch_x(c + 2)

            @pl.when(jnp.logical_and(t == 0, c + 1 < chunks))
            def _():
                wait_x(c + 1)

            terms(c, t)

            @pl.when(c + 1 < chunks)
            def _():
                project(c + 1, t)

        trail(i)

    for k in range(STAGE):
        stage_copy(pieces - STAGE + k).wait_send()
    pltpu.make_async_copy(sums, sums, sum_sem).wait()

    @pl.when(place == 2)
    def _():
        pltpu.make_async_copy(sums, sums, spread_sem).wait()

    @pl.when(place == 1)
    def _():
        pltpu.make_async_copy(high, high, pass_sem).wait()

    pltpu.make_async_copy(sums, sums, y_sem).wait()
    pltpu.make_async_copy(sums, sums, give_sem).wait()
    pltpu.make_async_copy(sums, sums, take_sem).wait()


def put_out(y_vmem, y_hbm, sem):
    rows = y_vmem.shape[0] // OUT_COPIES
    for k in range(OUT_COPIES):
        part = pl.ds(k * rows, rows)
        pltpu.make_async_copy(y_vmem.at[part], y_hbm.at[part], sem).start()
    pltpu.make_async_copy(y_vmem, y_hbm, sem).wait()


def block(x, w_gate, w_up, w_down, chunk=CHUNK, tiles=TILES):
    rows, depth = x.shape
    units = w_gate.shape[1]
    pieces = rows // 2 // chunk * tiles
    piece = (chunk, depth // tiles)
    messages = pieces * PARTS
    buffers = pltpu.VMEM((messages, chunk, depth // tiles // PARTS), jnp.bfloat16)
    dma = pltpu.SemaphoreType.DMA
    anywhere = pl.BlockSpec(memory_space=pl.ANY)
    y = pl.pallas_call(
        functools.partial(kernel, chunk, tiles),
        out_shape=pltpu.VMEM((rows, depth), jnp.bfloat16),
        in_specs=[anywhere] * 4,
        out_specs=anywhere,
        scratch_shapes=[
            pltpu.VMEM((depth, units), jnp.bfloat16),
            pltpu.VMEM((depth, units), jnp.bfloat16),
            pltpu.VMEM((units, depth), jnp.bfloat16),
            pltpu.VMEM((2, 2 * chunk, depth), jnp.bfloat16),
            pltpu.VMEM((2, 2 * chunk, units), jnp.bfloat16),
            pltpu.VMEM((2 * chunk, units), jnp.float32),
            pltpu.VMEM((2 * chunk, units), jnp.float32),
            pltpu.VMEM((RING,) + piece, jnp.float32),
            pltpu.VMEM((STAGE,) + piece, jnp.bfloat16),
            pltpu.VMEM((pieces,) + piece, jnp.bfloat16), buffers, buffers, buffers,
            dma((2,)), dma((HEAD,)), dma((HEAD,)), dma((tiles,)), dma((STAGE,)),
            dma((pieces,)), dma((messages,)), dma((messages,)),
            dma, dma, dma, dma, dma, dma,
        ],
        compiler_params=pltpu.CompilerParams(
            collective_id=0, has_side_effects=True, vmem_limit_bytes=54_000_000
        ),
    )(x, w_gate, w_up, w_down)
    return pl.pallas_call(
        put_out,
        out_shape=jax.ShapeDtypeStruct((rows, depth), jnp.bfloat16),
        in_specs=[anywhere],
        out_specs=anywhere,
        scratch_shapes=[dma],
        compiler_params=pltpu.CompilerParams(vmem_limit_bytes=OUT_LIMIT),
    )(y)


def solution(mesh):
    return jax.shard_map(
        block,
        mesh=mesh,
        in_specs=(P("dp", None), P(None, "tp"), P(None, "tp"), P("tp", None)),
        out_specs=P("dp", None),
        check_vma=False,
    )
```

```python
import functools

import jax
import jax.numpy as jnp
from jax import lax
from jax.experimental import pallas as pl
from jax.experimental.pallas import tpu as pltpu
from jax.sharding import PartitionSpec as P

MESH = pl.DeviceIdType.MESH
CHIPS = 4
CHUNK = 64
TILES = 4
RING = 16
STAGE = 4
OUT_COPIES = 16
OUT_LIMIT = 1_000_000
SUM_LAG = ((0, 2, 5, 4), (0, 2, 5, 4))
DONE_LAG = ((24, 6, 24, 24), (24, 6, 24, 24))
PARTS = 1
HEAD = 6
OUT_COPIES = 16
OUT_LIMIT = 1_000_000
SUM_LAG = ((0, 2, 5, 4), (0, 2, 5, 4))
DONE_LAG = ((24, 6, 24, 24), (24, 6, 24, 24))
PARTS = 1
HEAD = 6
AHEAD = 5
DOWN_AT = 2


def by_place(core, place, rows):
    result = jnp.int32(rows[-1][-1])
    for k, row in enumerate(rows):
        for j, value in enumerate(row):
            result = jnp.where(jnp.logical_and(core == k, place == j), jnp.int32(value), result)
    return result


LONGEST = max(max(row) for row in SUM_LAG + DONE_LAG)


def kernel(
    chunk, tiles, x_hbm, gate_hbm, up_hbm, down_hbm, y_hbm,
    gate_w, up_w, down_w, x_buf, hidden, first_gate, first_up, own, stage, theirs, low, high, sums,
    x_sem, gate_sem, up_sem, down_sem, stage_sem, theirs_sem, low_sem, high_sem,
    sum_sem, spread_sem, pass_sem, y_sem, give_sem, take_sem,
):
    rows, depth = x_hbm.shape
    units = gate_hbm.shape[1]
    half = rows // 2
    chunks = half // chunk
    pieces = chunks * tiles
    unit_tile = units // tiles
    col_tile = depth // tiles

    me = lax.axis_index("tp")
    chip, core = me // 2, me % 2
    place = jnp.where(core == 1, chip, CHIPS - 1 - chip)

    def at_place(k):
        return {"tp": jnp.where(core == 1, k, CHIPS - 1 - k) * 2 + core}

    other = {"tp": me + 1 - 2 * core}
    before, after = at_place(place - 1), at_place(place + 1)
    inner = jnp.logical_or(place == 1, place == 2)

    barrier = pltpu.get_barrier_semaphore()
    pl.semaphore_signal(barrier, inc=1, device_id=other, device_id_type=MESH)

    @pl.when(place > 0)
    def _():
        pl.semaphore_signal(barrier, inc=1, device_id=before, device_id_type=MESH)

    @pl.when(place < CHIPS - 1)
    def _():
        pl.semaphore_signal(barrier, inc=1, device_id=after, device_id_type=MESH)

    def x_rows(which, c):
        return x_hbm.at[pl.ds(pl.multiple_of(which * half + c * chunk, chunk), chunk), :]

    def fetch_x(c):
        slot = lax.rem(c, 2)
        pltpu.make_async_copy(x_rows(core, c), x_buf.at[slot, pl.ds(0, chunk)], x_sem.at[slot]).start()
        pltpu.make_async_copy(x_rows(1 - core, c), x_buf.at[slot, pl.ds(chunk, chunk)], x_sem.at[slot]).start()

    def wait_x(c):
        slot = lax.rem(c, 2)
        pltpu.make_async_copy(x_hbm.at[pl.ds(0, 2 * chunk), :], x_buf.at[slot], x_sem.at[slot]).wait()

    depth_tile = depth // HEAD
    part_tile = col_tile // PARTS

    def unit_slice(t):
        return pl.ds(pl.multiple_of(t * unit_tile, unit_tile), unit_tile)

    def depth_slice(k):
        return pl.ds(pl.multiple_of(k * depth_tile, depth_tile), depth_tile)

    def col_slice(t):
        return pl.ds(pl.multiple_of(t * col_tile, col_tile), col_tile)

    def gate_copy(k):
        return pltpu.make_async_copy(gate_hbm.at[depth_slice(k)], gate_w.at[depth_slice(k)], gate_sem.at[k])

    def up_copy(k):
        return pltpu.make_async_copy(up_hbm.at[depth_slice(k)], up_w.at[depth_slice(k)], up_sem.at[k])

    def down_copy(t):
        return pltpu.make_async_copy(down_hbm.at[:, col_slice(t)], down_w.at[:, col_slice(t)], down_sem.at[t])

    def dot(a, b):
        return jnp.dot(a, b, preferred_element_type=jnp.float32)

    def activate(gate, up):
        return (jax.nn.silu(gate) * up).astype(jnp.bfloat16)

    def project(c, t):
        slot = lax.rem(c, 2)
        xs = x_buf[slot]
        hidden[slot, :, unit_slice(t)] = activate(dot(xs, gate_w[:, unit_slice(t)]), dot(xs, up_w[:, unit_slice(t)]))

    fetch_x(0)
    @pl.loop(0, HEAD)
    def _(k):
        gate_copy(k).start()
        up_copy(k).start()

    @pl.loop(0, tiles)
    def _(t):
        down_copy(t).start()

    fetch_x(1)

    def stage_copy(i):
        slot = lax.rem(i, STAGE)
        return pltpu.make_async_remote_copy(
            src_ref=stage.at[slot], dst_ref=theirs.at[i], send_sem=stage_sem.at[slot], recv_sem=theirs_sem.at[i],
            device_id=other, device_id_type=MESH,
        )

    def terms(c, t):
        i = c * tiles + t
        term = dot(hidden[lax.rem(c, 2)], down_w[:, col_slice(t)])

        @pl.when(i >= STAGE)
        def _():
            stage_copy(i - STAGE).wait_send()

        stage[lax.rem(i, STAGE)] = term[chunk:].astype(jnp.bfloat16)
        stage_copy(i).start()
        own[lax.rem(i, RING)] = term[:chunk]

    def low_copy(p):
        return pltpu.make_async_remote_copy(
            src_ref=sums.at[p], dst_ref=low.at[p], send_sem=sum_sem, recv_sem=low_sem.at[p],
            device_id=after, device_id_type=MESH,
        )

    def high_copy(p):
        return pltpu.make_async_remote_copy(
            src_ref=sums.at[p], dst_ref=high.at[p], send_sem=sum_sem, recv_sem=high_sem.at[p],
            device_id=before, device_id_type=MESH,
        )

    def spread_copy(p):
        return pltpu.make_async_remote_copy(
            src_ref=sums.at[p], dst_ref=high.at[p], send_sem=spread_sem, recv_sem=high_sem.at[p],
            device_id=after, device_id_type=MESH,
        )

    def pass_copy(p):
        return pltpu.make_async_remote_copy(
            src_ref=high.at[p], dst_ref=high.at[p], send_sem=pass_sem, recv_sem=high_sem.at[p],
            device_id=before, device_id_type=MESH,
        )

    def deliver(src, m):
        p = m // PARTS
        c, column = p // tiles, lax.rem(p, tiles) * col_tile + lax.rem(m, PARTS) * part_tile
        block = y_hbm.at[
            pl.ds(pl.multiple_of(core * half + c * chunk, chunk), chunk),
            pl.ds(pl.multiple_of(column, part_tile), part_tile),
        ]
        pltpu.make_async_remote_copy(
            src_ref=src, dst_ref=block, send_sem=give_sem, recv_sem=take_sem, device_id=other, device_id_type=MESH,
        ).start()
        pltpu.make_async_copy(src, block, y_sem).start()

    def combine(p):
        pltpu.make_async_copy(theirs.at[p], theirs.at[p], theirs_sem.at[p]).wait()
        for part in range(PARTS):
            combine_part(p, part)

    def combine_part(p, part):
        m = p * PARTS + part
        columns = slice(part * part_tile, (part + 1) * part_tile)

        def here():
            return own[lax.rem(p, RING), :, columns] + theirs[p, :, columns].astype(jnp.float32)

        @pl.when(jnp.logical_not(inner))
        def _():
            sums[m] = here().astype(jnp.bfloat16)

        @pl.when(inner)
        def _():
            pltpu.make_async_copy(low.at[m], low.at[m], low_sem.at[m]).wait()

        @pl.when(place == 1)
        def _():
            sums[m] = (here() + low[m].astype(jnp.float32)).astype(jnp.bfloat16)

        @pl.when(place == 2)
        def _():
            pltpu.make_async_copy(high.at[m], high.at[m], high_sem.at[m]).wait()
            sums[m] = (here() + low[m].astype(jnp.float32) + high[m].astype(jnp.float32)).astype(jnp.bfloat16)

        @pl.when(place < 2)
        def _():
            low_copy(m).start()

        @pl.when(place >= 2)
        def _():
            high_copy(m).start()

        @pl.when(place == 2)
        def _():
            spread_copy(m).start()
            deliver(sums.at[m], m)

    def finish(p):
        for part in range(PARTS):
            m = p * PARTS + part
            pltpu.make_async_copy(high.at[m], high.at[m], high_sem.at[m]).wait()

            @pl.when(place == 1)
            def _():
                pass_copy(m).start()

            deliver(high.at[m], m)

    sum_lag = by_place(core, place, SUM_LAG)
    done_lag = by_place(core, place, DONE_LAG)

    def trail(i):
        p = i - sum_lag

        @pl.when(jnp.logical_and(p >= 0, p < pieces))
        def _():
            combine(p)

        d = i - done_lag

        @pl.when(jnp.logical_and(jnp.logical_and(d >= 0, d < pieces), place != 2))
        def _():
            finish(d)

    wait_x(0)

    @pl.loop(0, HEAD)
    def _(k):
        gate_copy(k).wait()
        up_copy(k).wait()

        xs = x_buf[0, :, depth_slice(k)]
        gate = dot(xs, gate_w[depth_slice(k)])
        up = dot(xs, up_w[depth_slice(k)])

        @pl.when(k == 0)
        def _():
            first_gate[...] = gate
            first_up[...] = up

        @pl.when(k > 0)
        def _():
            first_gate[...] += gate
            first_up[...] += up

    hidden[0] = activate(first_gate[...], first_up[...])
    pl.semaphore_wait(barrier, jnp.where(inner, 3, 2))

    @pl.loop(0, pieces + LONGEST)
    def _(i):
        c, t = i // tiles, lax.rem(i, tiles)

        @pl.when(i < pieces)
        def _():
            @pl.when(c == 0)
            def _():
                down_copy(t).wait()

            @pl.when(jnp.logical_and(t == 0, c + 2 < chunks))
            def _():
                fetch_x(c + 2)

            @pl.when(jnp.logical_and(t == 0, c + 1 < chunks))
            def _():
                wait_x(c + 1)

            terms(c, t)

            @pl.when(c + 1 < chunks)
            def _():
                project(c + 1, t)

        trail(i)

    for k in range(STAGE):
        stage_copy(pieces - STAGE + k).wait_send()
    pltpu.make_async_copy(sums, sums, sum_sem).wait()

    @pl.when(place == 2)
    def _():
        pltpu.make_async_copy(sums, sums, spread_sem).wait()

    @pl.when(place == 1)
    def _():
        pltpu.make_async_copy(high, high, pass_sem).wait()

    pltpu.make_async_copy(sums, sums, y_sem).wait()
    pltpu.make_async_copy(sums, sums, give_sem).wait()
    pltpu.make_async_copy(sums, sums, take_sem).wait()


def put_out(y_vmem, y_hbm, sem):
    rows = y_vmem.shape[0] // OUT_COPIES
    for k in range(OUT_COPIES):
        part = pl.ds(k * rows, rows)
        pltpu.make_async_copy(y_vmem.at[part], y_hbm.at[part], sem).start()
    pltpu.make_async_copy(y_vmem, y_hbm, sem).wait()


def block(x, w_gate, w_up, w_down, chunk=CHUNK, tiles=TILES):
    rows, depth = x.shape
    units = w_gate.shape[1]
    pieces = rows // 2 // chunk * tiles
    piece = (chunk, depth // tiles)
    messages = pieces * PARTS
    buffers = pltpu.VMEM((messages, chunk, depth // tiles // PARTS), jnp.bfloat16)
    dma = pltpu.SemaphoreType.DMA
    anywhere = pl.BlockSpec(memory_space=pl.ANY)
    y = pl.pallas_call(
        functools.partial(kernel, chunk, tiles),
        out_shape=pltpu.VMEM((rows, depth), jnp.bfloat16),
        in_specs=[anywhere] * 4,
        out_specs=anywhere,
        scratch_shapes=[
            pltpu.VMEM((depth, units), jnp.bfloat16),
            pltpu.VMEM((depth, units), jnp.bfloat16),
            pltpu.VMEM((units, depth), jnp.bfloat16),
            pltpu.VMEM((2, 2 * chunk, depth), jnp.bfloat16),
            pltpu.VMEM((2, 2 * chunk, units), jnp.bfloat16),
            pltpu.VMEM((2 * chunk, units), jnp.float32),
            pltpu.VMEM((2 * chunk, units), jnp.float32),
            pltpu.VMEM((RING,) + piece, jnp.float32),
            pltpu.VMEM((STAGE,) + piece, jnp.bfloat16),
            pltpu.VMEM((pieces,) + piece, jnp.bfloat16), buffers, buffers, buffers,
            dma((2,)), dma((HEAD,)), dma((HEAD,)), dma((tiles,)), dma((STAGE,)),
            dma((pieces,)), dma((messages,)), dma((messages,)),
            dma, dma, dma, dma, dma, dma,
        ],
        compiler_params=pltpu.CompilerParams(
            collective_id=0, has_side_effects=True, vmem_limit_bytes=54_000_000
        ),
    )(x, w_gate, w_up, w_down)
    return pl.pallas_call(
        put_out,
        out_shape=jax.ShapeDtypeStruct((rows, depth), jnp.bfloat16),
        in_specs=[anywhere],
        out_specs=anywhere,
        scratch_shapes=[dma],
        compiler_params=pltpu.CompilerParams(vmem_limit_bytes=OUT_LIMIT),
    )(y)


def solution(mesh):
    return jax.shard_map(
        block,
        mesh=mesh,
        in_specs=(P("dp", None), P(None, "tp"), P(None, "tp"), P("tp", None)),
        out_specs=P("dp", None),
        check_vma=False,
    )
```

```python
import functools

import jax
import jax.numpy as jnp
from jax import lax
from jax.experimental import pallas as pl
from jax.experimental.pallas import tpu as pltpu
from jax.sharding import PartitionSpec as P

MESH = pl.DeviceIdType.MESH
CHIPS = 4
CHUNK = 64
TILES = 4
RING = 16
STAGE = 4
OUT_COPIES = 16
OUT_LIMIT = 1_000_000
SUM_LAG = ((0, 2, 5, 4), (0, 2, 5, 4))
DONE_LAG = ((24, 6, 24, 24), (24, 6, 24, 24))
PARTS = 1
HEAD = 6
AHEAD = 4
DOWN_AT = 3


def by_place(core, place, rows):
    result = jnp.int32(rows[-1][-1])
    for k, row in enumerate(rows):
        for j, value in enumerate(row):
            result = jnp.where(jnp.logical_and(core == k, place == j), jnp.int32(value), result)
    return result


LONGEST = max(max(row) for row in SUM_LAG + DONE_LAG)


def kernel(
    chunk, tiles, x_hbm, gate_hbm, up_hbm, down_hbm, y_hbm,
    gate_w, up_w, down_w, x_buf, hidden, first_gate, first_up, own, stage, theirs, low, high, sums,
    x_sem, gate_sem, up_sem, down_sem, stage_sem, theirs_sem, low_sem, high_sem,
    sum_sem, spread_sem, pass_sem, y_sem, give_sem, take_sem,
):
    rows, depth = x_hbm.shape
    units = gate_hbm.shape[1]
    half = rows // 2
    chunks = half // chunk
    pieces = chunks * tiles
    unit_tile = units // tiles
    col_tile = depth // tiles

    me = lax.axis_index("tp")
    chip, core = me // 2, me % 2
    place = jnp.where(core == 1, chip, CHIPS - 1 - chip)

    def at_place(k):
        return {"tp": jnp.where(core == 1, k, CHIPS - 1 - k) * 2 + core}

    other = {"tp": me + 1 - 2 * core}
    before, after = at_place(place - 1), at_place(place + 1)
    inner = jnp.logical_or(place == 1, place == 2)

    barrier = pltpu.get_barrier_semaphore()
    pl.semaphore_signal(barrier, inc=1, device_id=other, device_id_type=MESH)

    @pl.when(place > 0)
    def _():
        pl.semaphore_signal(barrier, inc=1, device_id=before, device_id_type=MESH)

    @pl.when(place < CHIPS - 1)
    def _():
        pl.semaphore_signal(barrier, inc=1, device_id=after, device_id_type=MESH)

    def x_rows(which, c):
        return x_hbm.at[pl.ds(pl.multiple_of(which * half + c * chunk, chunk), chunk), :]

    def fetch_x(c):
        slot = lax.rem(c, 2)
        pltpu.make_async_copy(x_rows(core, c), x_buf.at[slot, pl.ds(0, chunk)], x_sem.at[slot]).start()
        pltpu.make_async_copy(x_rows(1 - core, c), x_buf.at[slot, pl.ds(chunk, chunk)], x_sem.at[slot]).start()

    def wait_x(c):
        slot = lax.rem(c, 2)
        pltpu.make_async_copy(x_hbm.at[pl.ds(0, 2 * chunk), :], x_buf.at[slot], x_sem.at[slot]).wait()

    depth_tile = depth // HEAD
    part_tile = col_tile // PARTS

    def unit_slice(t):
        return pl.ds(pl.multiple_of(t * unit_tile, unit_tile), unit_tile)

    def depth_slice(k):
        return pl.ds(pl.multiple_of(k * depth_tile, depth_tile), depth_tile)

    def col_slice(t):
        return pl.ds(pl.multiple_of(t * col_tile, col_tile), col_tile)

    def gate_copy(k):
        return pltpu.make_async_copy(gate_hbm.at[depth_slice(k)], gate_w.at[depth_slice(k)], gate_sem.at[k])

    def up_copy(k):
        return pltpu.make_async_copy(up_hbm.at[depth_slice(k)], up_w.at[depth_slice(k)], up_sem.at[k])

    def down_copy(t):
        return pltpu.make_async_copy(down_hbm.at[:, col_slice(t)], down_w.at[:, col_slice(t)], down_sem.at[t])

    def dot(a, b):
        return jnp.dot(a, b, preferred_element_type=jnp.float32)

    def activate(gate, up):
        return (jax.nn.silu(gate) * up).astype(jnp.bfloat16)

    def project(c, t):
        slot = lax.rem(c, 2)
        xs = x_buf[slot]
        hidden[slot, :, unit_slice(t)] = activate(dot(xs, gate_w[:, unit_slice(t)]), dot(xs, up_w[:, unit_slice(t)]))

    fetch_x(0)
    @pl.loop(0, AHEAD)
    def _(k):
        gate_copy(k).start()
        up_copy(k).start()

    def stage_copy(i):
        slot = lax.rem(i, STAGE)
        return pltpu.make_async_remote_copy(
            src_ref=stage.at[slot], dst_ref=theirs.at[i], send_sem=stage_sem.at[slot], recv_sem=theirs_sem.at[i],
            device_id=other, device_id_type=MESH,
        )

    def terms(c, t):
        i = c * tiles + t
        term = dot(hidden[lax.rem(c, 2)], down_w[:, col_slice(t)])

        @pl.when(i >= STAGE)
        def _():
            stage_copy(i - STAGE).wait_send()

        stage[lax.rem(i, STAGE)] = term[chunk:].astype(jnp.bfloat16)
        stage_copy(i).start()
        own[lax.rem(i, RING)] = term[:chunk]

    def low_copy(p):
        return pltpu.make_async_remote_copy(
            src_ref=sums.at[p], dst_ref=low.at[p], send_sem=sum_sem, recv_sem=low_sem.at[p],
            device_id=after, device_id_type=MESH,
        )

    def high_copy(p):
        return pltpu.make_async_remote_copy(
            src_ref=sums.at[p], dst_ref=high.at[p], send_sem=sum_sem, recv_sem=high_sem.at[p],
            device_id=before, device_id_type=MESH,
        )

    def spread_copy(p):
        return pltpu.make_async_remote_copy(
            src_ref=sums.at[p], dst_ref=high.at[p], send_sem=spread_sem, recv_sem=high_sem.at[p],
            device_id=after, device_id_type=MESH,
        )

    def pass_copy(p):
        return pltpu.make_async_remote_copy(
            src_ref=high.at[p], dst_ref=high.at[p], send_sem=pass_sem, recv_sem=high_sem.at[p],
            device_id=before, device_id_type=MESH,
        )

    def deliver(src, m):
        p = m // PARTS
        c, column = p // tiles, lax.rem(p, tiles) * col_tile + lax.rem(m, PARTS) * part_tile
        block = y_hbm.at[
            pl.ds(pl.multiple_of(core * half + c * chunk, chunk), chunk),
            pl.ds(pl.multiple_of(column, part_tile), part_tile),
        ]
        pltpu.make_async_remote_copy(
            src_ref=src, dst_ref=block, send_sem=give_sem, recv_sem=take_sem, device_id=other, device_id_type=MESH,
        ).start()
        pltpu.make_async_copy(src, block, y_sem).start()

    def combine(p):
        pltpu.make_async_copy(theirs.at[p], theirs.at[p], theirs_sem.at[p]).wait()
        for part in range(PARTS):
            combine_part(p, part)

    def combine_part(p, part):
        m = p * PARTS + part
        columns = slice(part * part_tile, (part + 1) * part_tile)

        def here():
            return own[lax.rem(p, RING), :, columns] + theirs[p, :, columns].astype(jnp.float32)

        @pl.when(jnp.logical_not(inner))
        def _():
            sums[m] = here().astype(jnp.bfloat16)

        @pl.when(inner)
        def _():
            pltpu.make_async_copy(low.at[m], low.at[m], low_sem.at[m]).wait()

        @pl.when(place == 1)
        def _():
            sums[m] = (here() + low[m].astype(jnp.float32)).astype(jnp.bfloat16)

        @pl.when(place == 2)
        def _():
            pltpu.make_async_copy(high.at[m], high.at[m], high_sem.at[m]).wait()
            sums[m] = (here() + low[m].astype(jnp.float32) + high[m].astype(jnp.float32)).astype(jnp.bfloat16)

        @pl.when(place < 2)
        def _():
            low_copy(m).start()

        @pl.when(place >= 2)
        def _():
            high_copy(m).start()

        @pl.when(place == 2)
        def _():
            spread_copy(m).start()
            deliver(sums.at[m], m)

    def finish(p):
        for part in range(PARTS):
            m = p * PARTS + part
            pltpu.make_async_copy(high.at[m], high.at[m], high_sem.at[m]).wait()

            @pl.when(place == 1)
            def _():
                pass_copy(m).start()

            deliver(high.at[m], m)

    sum_lag = by_place(core, place, SUM_LAG)
    done_lag = by_place(core, place, DONE_LAG)

    def trail(i):
        p = i - sum_lag

        @pl.when(jnp.logical_and(p >= 0, p < pieces))
        def _():
            combine(p)

        d = i - done_lag

        @pl.when(jnp.logical_and(jnp.logical_and(d >= 0, d < pieces), place != 2))
        def _():
            finish(d)

    wait_x(0)

    @pl.loop(0, HEAD)
    def _(k):
        gate_copy(k).wait()
        up_copy(k).wait()

        @pl.when(k + AHEAD < HEAD)
        def _():
            gate_copy(k + AHEAD).start()
            up_copy(k + AHEAD).start()

        @pl.when(k == DOWN_AT)
        def _():
            for t in range(tiles):
                down_copy(t).start()
            fetch_x(1)

        xs = x_buf[0, :, depth_slice(k)]
        gate = dot(xs, gate_w[depth_slice(k)])
        up = dot(xs, up_w[depth_slice(k)])

        @pl.when(k == 0)
        def _():
            first_gate[...] = gate
            first_up[...] = up

        @pl.when(k > 0)
        def _():
            first_gate[...] += gate
            first_up[...] += up

    hidden[0] = activate(first_gate[...], first_up[...])
    pl.semaphore_wait(barrier, jnp.where(inner, 3, 2))

    @pl.loop(0, pieces + LONGEST)
    def _(i):
        c, t = i // tiles, lax.rem(i, tiles)

        @pl.when(i < pieces)
        def _():
            @pl.when(c == 0)
            def _():
                down_copy(t).wait()

            @pl.when(jnp.logical_and(t == 0, c + 2 < chunks))
            def _():
                fetch_x(c + 2)

            @pl.when(jnp.logical_and(t == 0, c + 1 < chunks))
            def _():
                wait_x(c + 1)

            terms(c, t)

            @pl.when(c + 1 < chunks)
            def _():
                project(c + 1, t)

        trail(i)

    for k in range(STAGE):
        stage_copy(pieces - STAGE + k).wait_send()
    pltpu.make_async_copy(sums, sums, sum_sem).wait()

    @pl.when(place == 2)
    def _():
        pltpu.make_async_copy(sums, sums, spread_sem).wait()

    @pl.when(place == 1)
    def _():
        pltpu.make_async_copy(high, high, pass_sem).wait()

    pltpu.make_async_copy(sums, sums, y_sem).wait()
    pltpu.make_async_copy(sums, sums, give_sem).wait()
    pltpu.make_async_copy(sums, sums, take_sem).wait()


def put_out(y_vmem, y_hbm, sem):
    rows = y_vmem.shape[0] // OUT_COPIES
    for k in range(OUT_COPIES):
        part = pl.ds(k * rows, rows)
        pltpu.make_async_copy(y_vmem.at[part], y_hbm.at[part], sem).start()
    pltpu.make_async_copy(y_vmem, y_hbm, sem).wait()


def block(x, w_gate, w_up, w_down, chunk=CHUNK, tiles=TILES):
    rows, depth = x.shape
    units = w_gate.shape[1]
    pieces = rows // 2 // chunk * tiles
    piece = (chunk, depth // tiles)
    messages = pieces * PARTS
    buffers = pltpu.VMEM((messages, chunk, depth // tiles // PARTS), jnp.bfloat16)
    dma = pltpu.SemaphoreType.DMA
    anywhere = pl.BlockSpec(memory_space=pl.ANY)
    y = pl.pallas_call(
        functools.partial(kernel, chunk, tiles),
        out_shape=pltpu.VMEM((rows, depth), jnp.bfloat16),
        in_specs=[anywhere] * 4,
        out_specs=anywhere,
        scratch_shapes=[
            pltpu.VMEM((depth, units), jnp.bfloat16),
            pltpu.VMEM((depth, units), jnp.bfloat16),
            pltpu.VMEM((units, depth), jnp.bfloat16),
            pltpu.VMEM((2, 2 * chunk, depth), jnp.bfloat16),
            pltpu.VMEM((2, 2 * chunk, units), jnp.bfloat16),
            pltpu.VMEM((2 * chunk, units), jnp.float32),
            pltpu.VMEM((2 * chunk, units), jnp.float32),
            pltpu.VMEM((RING,) + piece, jnp.float32),
            pltpu.VMEM((STAGE,) + piece, jnp.bfloat16),
            pltpu.VMEM((pieces,) + piece, jnp.bfloat16), buffers, buffers, buffers,
            dma((2,)), dma((HEAD,)), dma((HEAD,)), dma((tiles,)), dma((STAGE,)),
            dma((pieces,)), dma((messages,)), dma((messages,)),
            dma, dma, dma, dma, dma, dma,
        ],
        compiler_params=pltpu.CompilerParams(
            collective_id=0, has_side_effects=True, vmem_limit_bytes=54_000_000
        ),
    )(x, w_gate, w_up, w_down)
    return pl.pallas_call(
        put_out,
        out_shape=jax.ShapeDtypeStruct((rows, depth), jnp.bfloat16),
        in_specs=[anywhere],
        out_specs=anywhere,
        scratch_shapes=[dma],
        compiler_params=pltpu.CompilerParams(vmem_limit_bytes=OUT_LIMIT),
    )(y)


def solution(mesh):
    return jax.shard_map(
        block,
        mesh=mesh,
        in_specs=(P("dp", None), P(None, "tp"), P(None, "tp"), P("tp", None)),
        out_specs=P("dp", None),
        check_vma=False,
    )
```

```python
import functools

import jax
import jax.numpy as jnp
from jax import lax
from jax.experimental import pallas as pl
from jax.experimental.pallas import tpu as pltpu
from jax.sharding import PartitionSpec as P

MESH = pl.DeviceIdType.MESH
CHIPS = 4
CHUNK = 64
TILES = 4
RING = 16
STAGE = 4
OUT_COPIES = 16
OUT_LIMIT = 1_000_000
SUM_LAG = ((0, 2, 5, 4), (0, 2, 5, 4))
DONE_LAG = ((24, 6, 24, 24), (24, 6, 24, 24))
LAST = 4
PARTS = 4
HEAD = 6
AHEAD = 4
DOWN_AT = 3


def by_place(core, place, rows):
    result = jnp.int32(rows[-1][-1])
    for k, row in enumerate(rows):
        for j, value in enumerate(row):
            result = jnp.where(jnp.logical_and(core == k, place == j), jnp.int32(value), result)
    return result


LONGEST = max(max(row) for row in SUM_LAG + DONE_LAG)


def kernel(
    chunk, tiles, x_hbm, gate_hbm, up_hbm, down_hbm, y_hbm,
    gate_w, up_w, down_w, x_buf, hidden, first_gate, first_up, own, stage, theirs, low, high, sums,
    x_sem, gate_sem, up_sem, down_sem, stage_sem, theirs_sem, low_sem, high_sem,
    sum_sem, spread_sem, pass_sem, y_sem, give_sem, take_sem,
):
    rows, depth = x_hbm.shape
    units = gate_hbm.shape[1]
    half = rows // 2
    chunks = half // chunk
    pieces = chunks * tiles
    unit_tile = units // tiles
    col_tile = depth // tiles

    me = lax.axis_index("tp")
    chip, core = me // 2, me % 2
    place = jnp.where(core == 1, chip, CHIPS - 1 - chip)

    def at_place(k):
        return {"tp": jnp.where(core == 1, k, CHIPS - 1 - k) * 2 + core}

    other = {"tp": me + 1 - 2 * core}
    before, after = at_place(place - 1), at_place(place + 1)
    inner = jnp.logical_or(place == 1, place == 2)

    barrier = pltpu.get_barrier_semaphore()
    pl.semaphore_signal(barrier, inc=1, device_id=other, device_id_type=MESH)

    @pl.when(place > 0)
    def _():
        pl.semaphore_signal(barrier, inc=1, device_id=before, device_id_type=MESH)

    @pl.when(place < CHIPS - 1)
    def _():
        pl.semaphore_signal(barrier, inc=1, device_id=after, device_id_type=MESH)

    def x_rows(which, c):
        return x_hbm.at[pl.ds(pl.multiple_of(which * half + c * chunk, chunk), chunk), :]

    def fetch_x(c):
        slot = lax.rem(c, 2)
        pltpu.make_async_copy(x_rows(core, c), x_buf.at[slot, pl.ds(0, chunk)], x_sem.at[slot]).start()
        pltpu.make_async_copy(x_rows(1 - core, c), x_buf.at[slot, pl.ds(chunk, chunk)], x_sem.at[slot]).start()

    def wait_x(c):
        slot = lax.rem(c, 2)
        pltpu.make_async_copy(x_hbm.at[pl.ds(0, 2 * chunk), :], x_buf.at[slot], x_sem.at[slot]).wait()

    depth_tile = depth // HEAD
    part_rows = chunk // PARTS

    def unit_slice(t):
        return pl.ds(pl.multiple_of(t * unit_tile, unit_tile), unit_tile)

    def depth_slice(k):
        return pl.ds(pl.multiple_of(k * depth_tile, depth_tile), depth_tile)

    def col_slice(t):
        return pl.ds(pl.multiple_of(t * col_tile, col_tile), col_tile)

    def gate_copy(k):
        return pltpu.make_async_copy(gate_hbm.at[depth_slice(k)], gate_w.at[depth_slice(k)], gate_sem.at[k])

    def up_copy(k):
        return pltpu.make_async_copy(up_hbm.at[depth_slice(k)], up_w.at[depth_slice(k)], up_sem.at[k])

    def down_copy(t):
        return pltpu.make_async_copy(down_hbm.at[:, col_slice(t)], down_w.at[:, col_slice(t)], down_sem.at[t])

    def dot(a, b):
        return jnp.dot(a, b, preferred_element_type=jnp.float32)

    def activate(gate, up):
        return (jax.nn.silu(gate) * up).astype(jnp.bfloat16)

    def project(c, t):
        slot = lax.rem(c, 2)
        xs = x_buf[slot]
        hidden[slot, :, unit_slice(t)] = activate(dot(xs, gate_w[:, unit_slice(t)]), dot(xs, up_w[:, unit_slice(t)]))

    fetch_x(0)
    @pl.loop(0, AHEAD)
    def _(k):
        gate_copy(k).start()
        up_copy(k).start()

    def stage_copy(i):
        slot = lax.rem(i, STAGE)
        return pltpu.make_async_remote_copy(
            src_ref=stage.at[slot], dst_ref=theirs.at[i], send_sem=stage_sem.at[slot], recv_sem=theirs_sem.at[i],
            device_id=other, device_id_type=MESH,
        )

    def terms(c, t):
        i = c * tiles + t
        term = dot(hidden[lax.rem(c, 2)], down_w[:, col_slice(t)])

        @pl.when(i >= STAGE)
        def _():
            stage_copy(i - STAGE).wait_send()

        stage[lax.rem(i, STAGE)] = term[chunk:].astype(jnp.bfloat16)
        stage_copy(i).start()
        own[lax.rem(i, RING)] = term[:chunk]

    def message(buffer, p, part):
        return buffer.at[p] if part is None else buffer.at[p, pl.ds(part * part_rows, part_rows)]

    def arrival(sems, p, part):
        return sems.at[pieces + (p - (pieces - LAST)) * (PARTS - 1) + part - 1 if part else p]

    def await_message(buffer, sems, p, part):
        ref = message(buffer, p, part)
        pltpu.make_async_copy(ref, ref, arrival(sems, p, part)).wait()

    def send(source, target, send_sem, sems, to, p, part):
        pltpu.make_async_remote_copy(
            src_ref=message(source, p, part), dst_ref=message(target, p, part), send_sem=send_sem,
            recv_sem=arrival(sems, p, part), device_id=to, device_id_type=MESH,
        ).start()

    def deliver(buffer, p, part):
        c, t = p // tiles, lax.rem(p, tiles)
        count = chunk if part is None else part_rows
        row = core * half + c * chunk + (part or 0) * part_rows
        src = message(buffer, p, part)
        block = y_hbm.at[
            pl.ds(pl.multiple_of(row, count), count), pl.ds(pl.multiple_of(t * col_tile, col_tile), col_tile)
        ]
        pltpu.make_async_remote_copy(
            src_ref=src, dst_ref=block, send_sem=give_sem, recv_sem=take_sem, device_id=other, device_id_type=MESH,
        ).start()
        pltpu.make_async_copy(src, block, y_sem).start()

    def combine_message(p, part):
        rows = slice(None) if part is None else slice(part * part_rows, (part + 1) * part_rows)

        def here():
            return own[lax.rem(p, RING), rows] + theirs[p, rows].astype(jnp.float32)

        @pl.when(jnp.logical_not(inner))
        def _():
            sums[p, rows] = here().astype(jnp.bfloat16)

        @pl.when(inner)
        def _():
            await_message(low, low_sem, p, part)

        @pl.when(place == 1)
        def _():
            sums[p, rows] = (here() + low[p, rows].astype(jnp.float32)).astype(jnp.bfloat16)

        @pl.when(place == 2)
        def _():
            await_message(high, high_sem, p, part)
            total = here() + low[p, rows].astype(jnp.float32) + high[p, rows].astype(jnp.float32)
            sums[p, rows] = total.astype(jnp.bfloat16)

        @pl.when(place < 2)
        def _():
            send(sums, low, sum_sem, low_sem, after, p, part)

        @pl.when(place >= 2)
        def _():
            send(sums, high, sum_sem, high_sem, before, p, part)

        @pl.when(place == 2)
        def _():
            send(sums, high, spread_sem, high_sem, after, p, part)
            deliver(sums, p, part)

    def finish_message(p, part):
        await_message(high, high_sem, p, part)

        @pl.when(place == 1)
        def _():
            send(high, high, pass_sem, high_sem, before, p, part)

        deliver(high, p, part)

    def by_message(p, action):
        @pl.when(p < pieces - LAST)
        def _():
            action(p, None)

        @pl.when(p >= pieces - LAST)
        def _():
            for part in range(PARTS):
                action(p, part)

    def combine(p):
        pltpu.make_async_copy(theirs.at[p], theirs.at[p], theirs_sem.at[p]).wait()
        by_message(p, combine_message)

    def finish(p):
        by_message(p, finish_message)

    sum_lag = by_place(core, place, SUM_LAG)
    done_lag = by_place(core, place, DONE_LAG)

    def trail(i):
        p = i - sum_lag

        @pl.when(jnp.logical_and(p >= 0, p < pieces))
        def _():
            combine(p)

        d = i - done_lag

        @pl.when(jnp.logical_and(jnp.logical_and(d >= 0, d < pieces), place != 2))
        def _():
            finish(d)

    wait_x(0)

    @pl.loop(0, HEAD)
    def _(k):
        gate_copy(k).wait()
        up_copy(k).wait()

        @pl.when(k + AHEAD < HEAD)
        def _():
            gate_copy(k + AHEAD).start()
            up_copy(k + AHEAD).start()

        @pl.when(k == DOWN_AT)
        def _():
            for t in range(tiles):
                down_copy(t).start()
            fetch_x(1)

        xs = x_buf[0, :, depth_slice(k)]
        gate = dot(xs, gate_w[depth_slice(k)])
        up = dot(xs, up_w[depth_slice(k)])

        @pl.when(k == 0)
        def _():
            first_gate[...] = gate
            first_up[...] = up

        @pl.when(k > 0)
        def _():
            first_gate[...] += gate
            first_up[...] += up

    hidden[0] = activate(first_gate[...], first_up[...])
    pl.semaphore_wait(barrier, jnp.where(inner, 3, 2))

    @pl.loop(0, pieces + LONGEST)
    def _(i):
        c, t = i // tiles, lax.rem(i, tiles)

        @pl.when(i < pieces)
        def _():
            @pl.when(c == 0)
            def _():
                down_copy(t).wait()

            @pl.when(jnp.logical_and(t == 0, c + 2 < chunks))
            def _():
                fetch_x(c + 2)

            @pl.when(jnp.logical_and(t == 0, c + 1 < chunks))
            def _():
                wait_x(c + 1)

            terms(c, t)

            @pl.when(c + 1 < chunks)
            def _():
                project(c + 1, t)

        trail(i)

    for k in range(STAGE):
        stage_copy(pieces - STAGE + k).wait_send()
    pltpu.make_async_copy(sums, sums, sum_sem).wait()

    @pl.when(place == 2)
    def _():
        pltpu.make_async_copy(sums, sums, spread_sem).wait()

    @pl.when(place == 1)
    def _():
        pltpu.make_async_copy(high, high, pass_sem).wait()

    pltpu.make_async_copy(sums, sums, y_sem).wait()
    pltpu.make_async_copy(sums, sums, give_sem).wait()
    pltpu.make_async_copy(sums, sums, take_sem).wait()


def put_out(y_vmem, y_hbm, sem):
    rows = y_vmem.shape[0] // OUT_COPIES
    for k in range(OUT_COPIES):
        part = pl.ds(k * rows, rows)
        pltpu.make_async_copy(y_vmem.at[part], y_hbm.at[part], sem).start(priority=k % 2)
    pltpu.make_async_copy(y_vmem, y_hbm, sem).wait()


def block(x, w_gate, w_up, w_down, chunk=CHUNK, tiles=TILES):
    rows, depth = x.shape
    units = w_gate.shape[1]
    pieces = rows // 2 // chunk * tiles
    piece = (chunk, depth // tiles)
    messages = pieces + LAST * (PARTS - 1)
    buffers = pltpu.VMEM((pieces,) + piece, jnp.bfloat16)
    dma = pltpu.SemaphoreType.DMA
    anywhere = pl.BlockSpec(memory_space=pl.ANY)
    y = pl.pallas_call(
        functools.partial(kernel, chunk, tiles),
        out_shape=pltpu.VMEM((rows, depth), jnp.bfloat16),
        in_specs=[anywhere] * 4,
        out_specs=anywhere,
        scratch_shapes=[
            pltpu.VMEM((depth, units), jnp.bfloat16),
            pltpu.VMEM((depth, units), jnp.bfloat16),
            pltpu.VMEM((units, depth), jnp.bfloat16),
            pltpu.VMEM((2, 2 * chunk, depth), jnp.bfloat16),
            pltpu.VMEM((2, 2 * chunk, units), jnp.bfloat16),
            pltpu.VMEM((2 * chunk, units), jnp.float32),
            pltpu.VMEM((2 * chunk, units), jnp.float32),
            pltpu.VMEM((RING,) + piece, jnp.float32),
            pltpu.VMEM((STAGE,) + piece, jnp.bfloat16),
            buffers, buffers, buffers, buffers,
            dma((2,)), dma((HEAD,)), dma((HEAD,)), dma((tiles,)), dma((STAGE,)),
            dma((pieces,)), dma((messages,)), dma((messages,)),
            dma, dma, dma, dma, dma, dma,
        ],
        compiler_params=pltpu.CompilerParams(
            collective_id=0, has_side_effects=True, vmem_limit_bytes=54_000_000
        ),
    )(x, w_gate, w_up, w_down)
    return pl.pallas_call(
        put_out,
        out_shape=jax.ShapeDtypeStruct((rows, depth), jnp.bfloat16),
        in_specs=[anywhere],
        out_specs=anywhere,
        scratch_shapes=[dma],
        compiler_params=pltpu.CompilerParams(vmem_limit_bytes=OUT_LIMIT),
    )(y)


def solution(mesh):
    return jax.shard_map(
        block,
        mesh=mesh,
        in_specs=(P("dp", None), P(None, "tp"), P(None, "tp"), P("tp", None)),
        out_specs=P("dp", None),
        check_vma=False,
    )
```

```python
import functools

import jax
import jax.numpy as jnp
from jax import lax
from jax.experimental import pallas as pl
from jax.experimental.pallas import tpu as pltpu
from jax.sharding import PartitionSpec as P

MESH = pl.DeviceIdType.MESH
CHIPS = 4
CHUNK = 64
TILES = 4
RING = 16
STAGE = 4
OUT_COPIES = 16
OUT_LIMIT = 1_000_000
SUM_LAG = ((0, 2, 5, 3), (0, 2, 5, 3))
DONE_LAG = ((24, 6, 24, 24), (24, 6, 24, 24))
PARTS = 1
HEAD = 6
AHEAD = 4
DOWN_AT = 3


def by_place(core, place, rows):
    result = jnp.int32(rows[-1][-1])
    for k, row in enumerate(rows):
        for j, value in enumerate(row):
            result = jnp.where(jnp.logical_and(core == k, place == j), jnp.int32(value), result)
    return result


LONGEST = max(max(row) for row in SUM_LAG + DONE_LAG)


def kernel(
    chunk, tiles, x_hbm, gate_hbm, up_hbm, down_hbm, y_hbm,
    gate_w, up_w, down_w, x_buf, hidden, first_gate, first_up, own, stage, theirs, low, high, sums,
    x_sem, gate_sem, up_sem, down_sem, stage_sem, theirs_sem, low_sem, high_sem,
    sum_sem, spread_sem, pass_sem, y_sem, give_sem, take_sem,
):
    rows, depth = x_hbm.shape
    units = gate_hbm.shape[1]
    half = rows // 2
    chunks = half // chunk
    pieces = chunks * tiles
    unit_tile = units // tiles
    col_tile = depth // tiles

    me = lax.axis_index("tp")
    chip, core = me // 2, me % 2
    place = jnp.where(core == 1, chip, CHIPS - 1 - chip)

    def at_place(k):
        return {"tp": jnp.where(core == 1, k, CHIPS - 1 - k) * 2 + core}

    other = {"tp": me + 1 - 2 * core}
    before, after = at_place(place - 1), at_place(place + 1)
    inner = jnp.logical_or(place == 1, place == 2)

    barrier = pltpu.get_barrier_semaphore()
    pl.semaphore_signal(barrier, inc=1, device_id=other, device_id_type=MESH)

    @pl.when(place > 0)
    def _():
        pl.semaphore_signal(barrier, inc=1, device_id=before, device_id_type=MESH)

    @pl.when(place < CHIPS - 1)
    def _():
        pl.semaphore_signal(barrier, inc=1, device_id=after, device_id_type=MESH)

    def x_rows(which, c):
        return x_hbm.at[pl.ds(pl.multiple_of(which * half + c * chunk, chunk), chunk), :]

    def fetch_x(c):
        slot = lax.rem(c, 2)
        pltpu.make_async_copy(x_rows(core, c), x_buf.at[slot, pl.ds(0, chunk)], x_sem.at[slot]).start()
        pltpu.make_async_copy(x_rows(1 - core, c), x_buf.at[slot, pl.ds(chunk, chunk)], x_sem.at[slot]).start()

    def wait_x(c):
        slot = lax.rem(c, 2)
        pltpu.make_async_copy(x_hbm.at[pl.ds(0, 2 * chunk), :], x_buf.at[slot], x_sem.at[slot]).wait()

    depth_tile = depth // HEAD
    part_tile = col_tile // PARTS

    def unit_slice(t):
        return pl.ds(pl.multiple_of(t * unit_tile, unit_tile), unit_tile)

    def depth_slice(k):
        return pl.ds(pl.multiple_of(k * depth_tile, depth_tile), depth_tile)

    def col_slice(t):
        return pl.ds(pl.multiple_of(t * col_tile, col_tile), col_tile)

    def gate_copy(k):
        return pltpu.make_async_copy(gate_hbm.at[depth_slice(k)], gate_w.at[depth_slice(k)], gate_sem.at[k])

    def up_copy(k):
        return pltpu.make_async_copy(up_hbm.at[depth_slice(k)], up_w.at[depth_slice(k)], up_sem.at[k])

    def down_copy(t):
        return pltpu.make_async_copy(down_hbm.at[:, col_slice(t)], down_w.at[:, col_slice(t)], down_sem.at[t])

    def dot(a, b):
        return jnp.dot(a, b, preferred_element_type=jnp.float32)

    def activate(gate, up):
        return (jax.nn.silu(gate) * up).astype(jnp.bfloat16)

    def project(c, t):
        slot = lax.rem(c, 2)
        xs = x_buf[slot]
        hidden[slot, :, unit_slice(t)] = activate(dot(xs, gate_w[:, unit_slice(t)]), dot(xs, up_w[:, unit_slice(t)]))

    fetch_x(0)
    @pl.loop(0, AHEAD)
    def _(k):
        gate_copy(k).start()
        up_copy(k).start()

    def stage_copy(i):
        slot = lax.rem(i, STAGE)
        return pltpu.make_async_remote_copy(
            src_ref=stage.at[slot], dst_ref=theirs.at[i], send_sem=stage_sem.at[slot], recv_sem=theirs_sem.at[i],
            device_id=other, device_id_type=MESH,
        )

    def terms(c, t):
        i = c * tiles + t
        term = dot(hidden[lax.rem(c, 2)], down_w[:, col_slice(t)])

        @pl.when(i >= STAGE)
        def _():
            stage_copy(i - STAGE).wait_send()

        stage[lax.rem(i, STAGE)] = term[chunk:].astype(jnp.bfloat16)
        stage_copy(i).start()
        own[lax.rem(i, RING)] = term[:chunk]

    def low_copy(p):
        return pltpu.make_async_remote_copy(
            src_ref=sums.at[p], dst_ref=low.at[p], send_sem=sum_sem, recv_sem=low_sem.at[p],
            device_id=after, device_id_type=MESH,
        )

    def high_copy(p):
        return pltpu.make_async_remote_copy(
            src_ref=sums.at[p], dst_ref=high.at[p], send_sem=sum_sem, recv_sem=high_sem.at[p],
            device_id=before, device_id_type=MESH,
        )

    def spread_copy(p):
        return pltpu.make_async_remote_copy(
            src_ref=sums.at[p], dst_ref=high.at[p], send_sem=spread_sem, recv_sem=high_sem.at[p],
            device_id=after, device_id_type=MESH,
        )

    def pass_copy(p):
        return pltpu.make_async_remote_copy(
            src_ref=high.at[p], dst_ref=high.at[p], send_sem=pass_sem, recv_sem=high_sem.at[p],
            device_id=before, device_id_type=MESH,
        )

    def deliver(src, m):
        p = m // PARTS
        c, column = p // tiles, lax.rem(p, tiles) * col_tile + lax.rem(m, PARTS) * part_tile
        block = y_hbm.at[
            pl.ds(pl.multiple_of(core * half + c * chunk, chunk), chunk),
            pl.ds(pl.multiple_of(column, part_tile), part_tile),
        ]
        pltpu.make_async_remote_copy(
            src_ref=src, dst_ref=block, send_sem=give_sem, recv_sem=take_sem, device_id=other, device_id_type=MESH,
        ).start()
        pltpu.make_async_copy(src, block, y_sem).start()

    def combine(p):
        pltpu.make_async_copy(theirs.at[p], theirs.at[p], theirs_sem.at[p]).wait()
        for part in range(PARTS):
            combine_part(p, part)

    def combine_part(p, part):
        m = p * PARTS + part
        columns = slice(part * part_tile, (part + 1) * part_tile)

        def here():
            return own[lax.rem(p, RING), :, columns] + theirs[p, :, columns].astype(jnp.float32)

        @pl.when(jnp.logical_not(inner))
        def _():
            sums[m] = here().astype(jnp.bfloat16)

        @pl.when(inner)
        def _():
            pltpu.make_async_copy(low.at[m], low.at[m], low_sem.at[m]).wait()

        @pl.when(place == 1)
        def _():
            sums[m] = (here() + low[m].astype(jnp.float32)).astype(jnp.bfloat16)

        @pl.when(place == 2)
        def _():
            pltpu.make_async_copy(high.at[m], high.at[m], high_sem.at[m]).wait()
            sums[m] = (here() + low[m].astype(jnp.float32) + high[m].astype(jnp.float32)).astype(jnp.bfloat16)

        @pl.when(place < 2)
        def _():
            low_copy(m).start()

        @pl.when(place >= 2)
        def _():
            high_copy(m).start()

        @pl.when(place == 2)
        def _():
            spread_copy(m).start()
            deliver(sums.at[m], m)

    def finish(p):
        for part in range(PARTS):
            m = p * PARTS + part
            pltpu.make_async_copy(high.at[m], high.at[m], high_sem.at[m]).wait()

            @pl.when(place == 1)
            def _():
                pass_copy(m).start()

            deliver(high.at[m], m)

    sum_lag = by_place(core, place, SUM_LAG)
    done_lag = by_place(core, place, DONE_LAG)

    def trail(i):
        p = i - sum_lag

        @pl.when(jnp.logical_and(p >= 0, p < pieces))
        def _():
            combine(p)

        d = i - done_lag

        @pl.when(jnp.logical_and(jnp.logical_and(d >= 0, d < pieces), place != 2))
        def _():
            finish(d)

    wait_x(0)

    @pl.loop(0, HEAD)
    def _(k):
        gate_copy(k).wait()
        up_copy(k).wait()

        @pl.when(k + AHEAD < HEAD)
        def _():
            gate_copy(k + AHEAD).start()
            up_copy(k + AHEAD).start()

        @pl.when(k == DOWN_AT)
        def _():
            for t in range(tiles):
                down_copy(t).start()
            fetch_x(1)

        xs = x_buf[0, :, depth_slice(k)]
        gate = dot(xs, gate_w[depth_slice(k)])
        up = dot(xs, up_w[depth_slice(k)])

        @pl.when(k == 0)
        def _():
            first_gate[...] = gate
            first_up[...] = up

        @pl.when(k > 0)
        def _():
            first_gate[...] += gate
            first_up[...] += up

    hidden[0] = activate(first_gate[...], first_up[...])
    pl.semaphore_wait(barrier, jnp.where(inner, 3, 2))

    def terms_of(i):
        @pl.when(i < tiles)
        def _():
            down_copy(i).wait()

        terms(i // tiles, lax.rem(i, tiles))

    terms_of(jnp.int32(0))

    @pl.loop(0, pieces + LONGEST)
    def _(i):
        c, t = i // tiles, lax.rem(i, tiles)

        @pl.when(jnp.logical_and(t == 0, c + 2 < chunks))
        def _():
            fetch_x(c + 2)

        @pl.when(jnp.logical_and(t == 0, c + 1 < chunks))
        def _():
            wait_x(c + 1)

        @pl.when(c + 1 < chunks)
        def _():
            project(c + 1, t)

        @pl.when(i + 1 < pieces)
        def _():
            terms_of(i + 1)

        trail(i)

    for k in range(STAGE):
        stage_copy(pieces - STAGE + k).wait_send()
    pltpu.make_async_copy(sums, sums, sum_sem).wait()

    @pl.when(place == 2)
    def _():
        pltpu.make_async_copy(sums, sums, spread_sem).wait()

    @pl.when(place == 1)
    def _():
        pltpu.make_async_copy(high, high, pass_sem).wait()

    pltpu.make_async_copy(sums, sums, y_sem).wait()
    pltpu.make_async_copy(sums, sums, give_sem).wait()
    pltpu.make_async_copy(sums, sums, take_sem).wait()


def put_out(y_vmem, y_hbm, sem):
    rows = y_vmem.shape[0] // OUT_COPIES
    for k in range(OUT_COPIES):
        part = pl.ds(k * rows, rows)
        pltpu.make_async_copy(y_vmem.at[part], y_hbm.at[part], sem).start()
    pltpu.make_async_copy(y_vmem, y_hbm, sem).wait()


def block(x, w_gate, w_up, w_down, chunk=CHUNK, tiles=TILES):
    rows, depth = x.shape
    units = w_gate.shape[1]
    pieces = rows // 2 // chunk * tiles
    piece = (chunk, depth // tiles)
    messages = pieces * PARTS
    buffers = pltpu.VMEM((messages, chunk, depth // tiles // PARTS), jnp.bfloat16)
    dma = pltpu.SemaphoreType.DMA
    anywhere = pl.BlockSpec(memory_space=pl.ANY)
    y = pl.pallas_call(
        functools.partial(kernel, chunk, tiles),
        out_shape=pltpu.VMEM((rows, depth), jnp.bfloat16),
        in_specs=[anywhere] * 4,
        out_specs=anywhere,
        scratch_shapes=[
            pltpu.VMEM((depth, units), jnp.bfloat16),
            pltpu.VMEM((depth, units), jnp.bfloat16),
            pltpu.VMEM((units, depth), jnp.bfloat16),
            pltpu.VMEM((2, 2 * chunk, depth), jnp.bfloat16),
            pltpu.VMEM((2, 2 * chunk, units), jnp.bfloat16),
            pltpu.VMEM((2 * chunk, units), jnp.float32),
            pltpu.VMEM((2 * chunk, units), jnp.float32),
            pltpu.VMEM((RING,) + piece, jnp.float32),
            pltpu.VMEM((STAGE,) + piece, jnp.bfloat16),
            pltpu.VMEM((pieces,) + piece, jnp.bfloat16), buffers, buffers, buffers,
            dma((2,)), dma((HEAD,)), dma((HEAD,)), dma((tiles,)), dma((STAGE,)),
            dma((pieces,)), dma((messages,)), dma((messages,)),
            dma, dma, dma, dma, dma, dma,
        ],
        compiler_params=pltpu.CompilerParams(
            collective_id=0, has_side_effects=True, vmem_limit_bytes=54_000_000
        ),
    )(x, w_gate, w_up, w_down)
    return pl.pallas_call(
        put_out,
        out_shape=jax.ShapeDtypeStruct((rows, depth), jnp.bfloat16),
        in_specs=[anywhere],
        out_specs=anywhere,
        scratch_shapes=[dma],
        compiler_params=pltpu.CompilerParams(vmem_limit_bytes=OUT_LIMIT),
    )(y)


def solution(mesh):
    return jax.shard_map(
        block,
        mesh=mesh,
        in_specs=(P("dp", None), P(None, "tp"), P(None, "tp"), P("tp", None)),
        out_specs=P("dp", None),
        check_vma=False,
    )
```

```python
import functools

import jax
import jax.numpy as jnp
from jax import lax
from jax.experimental import pallas as pl
from jax.experimental.pallas import tpu as pltpu
from jax.sharding import PartitionSpec as P

MESH = pl.DeviceIdType.MESH
CHIPS = 4
CHUNK = 64
TILES = 4
RING = 16
STAGE = 4
OUT_COPIES = 16
OUT_LIMIT = 1_000_000
SUM_LAG = ((0, 2, 5, 3), (0, 2, 5, 5))
DONE_LAG = ((24, 6, 24, 24), (24, 6, 24, 24))
PARTS = 1
HEAD = 6
AHEAD = 4
DOWN_AT = 3


def by_place(core, place, rows):
    result = jnp.int32(rows[-1][-1])
    for k, row in enumerate(rows):
        for j, value in enumerate(row):
            result = jnp.where(jnp.logical_and(core == k, place == j), jnp.int32(value), result)
    return result


LONGEST = max(max(row) for row in SUM_LAG + DONE_LAG)


def kernel(
    chunk, tiles, x_hbm, gate_hbm, up_hbm, down_hbm, y_hbm,
    gate_w, up_w, down_w, x_buf, hidden, first_gate, first_up, own, stage, theirs, low, high, sums,
    x_sem, gate_sem, up_sem, down_sem, stage_sem, theirs_sem, low_sem, high_sem,
    sum_sem, spread_sem, pass_sem, y_sem, give_sem, take_sem,
):
    rows, depth = x_hbm.shape
    units = gate_hbm.shape[1]
    half = rows // 2
    chunks = half // chunk
    pieces = chunks * tiles
    unit_tile = units // tiles
    col_tile = depth // tiles

    me = lax.axis_index("tp")
    chip, core = me // 2, me % 2
    place = jnp.where(core == 1, chip, CHIPS - 1 - chip)

    def at_place(k):
        return {"tp": jnp.where(core == 1, k, CHIPS - 1 - k) * 2 + core}

    other = {"tp": me + 1 - 2 * core}
    before, after = at_place(place - 1), at_place(place + 1)
    inner = jnp.logical_or(place == 1, place == 2)

    barrier = pltpu.get_barrier_semaphore()
    pl.semaphore_signal(barrier, inc=1, device_id=other, device_id_type=MESH)

    @pl.when(place > 0)
    def _():
        pl.semaphore_signal(barrier, inc=1, device_id=before, device_id_type=MESH)

    @pl.when(place < CHIPS - 1)
    def _():
        pl.semaphore_signal(barrier, inc=1, device_id=after, device_id_type=MESH)

    def x_rows(which, c):
        return x_hbm.at[pl.ds(pl.multiple_of(which * half + c * chunk, chunk), chunk), :]

    def fetch_x(c):
        slot = lax.rem(c, 2)
        pltpu.make_async_copy(x_rows(core, c), x_buf.at[slot, pl.ds(0, chunk)], x_sem.at[slot]).start()
        pltpu.make_async_copy(x_rows(1 - core, c), x_buf.at[slot, pl.ds(chunk, chunk)], x_sem.at[slot]).start()

    def wait_x(c):
        slot = lax.rem(c, 2)
        pltpu.make_async_copy(x_hbm.at[pl.ds(0, 2 * chunk), :], x_buf.at[slot], x_sem.at[slot]).wait()

    depth_tile = depth // HEAD
    part_tile = col_tile // PARTS

    def unit_slice(t):
        return pl.ds(pl.multiple_of(t * unit_tile, unit_tile), unit_tile)

    def depth_slice(k):
        return pl.ds(pl.multiple_of(k * depth_tile, depth_tile), depth_tile)

    def col_slice(t):
        return pl.ds(pl.multiple_of(t * col_tile, col_tile), col_tile)

    def gate_copy(k):
        return pltpu.make_async_copy(gate_hbm.at[depth_slice(k)], gate_w.at[depth_slice(k)], gate_sem.at[k])

    def up_copy(k):
        return pltpu.make_async_copy(up_hbm.at[depth_slice(k)], up_w.at[depth_slice(k)], up_sem.at[k])

    def down_copy(t):
        return pltpu.make_async_copy(down_hbm.at[:, col_slice(t)], down_w.at[:, col_slice(t)], down_sem.at[t])

    def dot(a, b):
        return jnp.dot(a, b, preferred_element_type=jnp.float32)

    def activate(gate, up):
        return (jax.nn.silu(gate) * up).astype(jnp.bfloat16)

    def project(c, t):
        slot = lax.rem(c, 2)
        xs = x_buf[slot]
        hidden[slot, :, unit_slice(t)] = activate(dot(xs, gate_w[:, unit_slice(t)]), dot(xs, up_w[:, unit_slice(t)]))

    fetch_x(0)
    @pl.loop(0, AHEAD)
    def _(k):
        gate_copy(k).start()
        up_copy(k).start()

    def stage_copy(i):
        slot = lax.rem(i, STAGE)
        return pltpu.make_async_remote_copy(
            src_ref=stage.at[slot], dst_ref=theirs.at[i], send_sem=stage_sem.at[slot], recv_sem=theirs_sem.at[i],
            device_id=other, device_id_type=MESH,
        )

    def terms(c, t):
        i = c * tiles + t
        term = dot(hidden[lax.rem(c, 2)], down_w[:, col_slice(t)])

        @pl.when(i >= STAGE)
        def _():
            stage_copy(i - STAGE).wait_send()

        stage[lax.rem(i, STAGE)] = term[chunk:].astype(jnp.bfloat16)
        stage_copy(i).start()
        own[lax.rem(i, RING)] = term[:chunk]

    def low_copy(p):
        return pltpu.make_async_remote_copy(
            src_ref=sums.at[p], dst_ref=low.at[p], send_sem=sum_sem, recv_sem=low_sem.at[p],
            device_id=after, device_id_type=MESH,
        )

    def high_copy(p):
        return pltpu.make_async_remote_copy(
            src_ref=sums.at[p], dst_ref=high.at[p], send_sem=sum_sem, recv_sem=high_sem.at[p],
            device_id=before, device_id_type=MESH,
        )

    def spread_copy(p):
        return pltpu.make_async_remote_copy(
            src_ref=sums.at[p], dst_ref=high.at[p], send_sem=spread_sem, recv_sem=high_sem.at[p],
            device_id=after, device_id_type=MESH,
        )

    def pass_copy(p):
        return pltpu.make_async_remote_copy(
            src_ref=high.at[p], dst_ref=high.at[p], send_sem=pass_sem, recv_sem=high_sem.at[p],
            device_id=before, device_id_type=MESH,
        )

    def deliver(src, m):
        p = m // PARTS
        c, column = p // tiles, lax.rem(p, tiles) * col_tile + lax.rem(m, PARTS) * part_tile
        block = y_hbm.at[
            pl.ds(pl.multiple_of(core * half + c * chunk, chunk), chunk),
            pl.ds(pl.multiple_of(column, part_tile), part_tile),
        ]
        pltpu.make_async_remote_copy(
            src_ref=src, dst_ref=block, send_sem=give_sem, recv_sem=take_sem, device_id=other, device_id_type=MESH,
        ).start()
        pltpu.make_async_copy(src, block, y_sem).start()

    def combine(p):
        pltpu.make_async_copy(theirs.at[p], theirs.at[p], theirs_sem.at[p]).wait()
        for part in range(PARTS):
            combine_part(p, part)

    def combine_part(p, part):
        m = p * PARTS + part
        columns = slice(part * part_tile, (part + 1) * part_tile)

        def here():
            return own[lax.rem(p, RING), :, columns] + theirs[p, :, columns].astype(jnp.float32)

        @pl.when(jnp.logical_not(inner))
        def _():
            sums[m] = here().astype(jnp.bfloat16)

        @pl.when(inner)
        def _():
            pltpu.make_async_copy(low.at[m], low.at[m], low_sem.at[m]).wait()

        @pl.when(place == 1)
        def _():
            sums[m] = (here() + low[m].astype(jnp.float32)).astype(jnp.bfloat16)

        @pl.when(place == 2)
        def _():
            pltpu.make_async_copy(high.at[m], high.at[m], high_sem.at[m]).wait()
            sums[m] = (here() + low[m].astype(jnp.float32) + high[m].astype(jnp.float32)).astype(jnp.bfloat16)

        @pl.when(place < 2)
        def _():
            low_copy(m).start()

        @pl.when(place >= 2)
        def _():
            high_copy(m).start()

        @pl.when(place == 2)
        def _():
            spread_copy(m).start()
            deliver(sums.at[m], m)

    def finish(p):
        for part in range(PARTS):
            m = p * PARTS + part
            pltpu.make_async_copy(high.at[m], high.at[m], high_sem.at[m]).wait()

            @pl.when(place == 1)
            def _():
                pass_copy(m).start()

            deliver(high.at[m], m)

    sum_lag = by_place(core, place, SUM_LAG)
    done_lag = by_place(core, place, DONE_LAG)

    def trail(i):
        p = i - sum_lag

        @pl.when(jnp.logical_and(p >= 0, p < pieces))
        def _():
            combine(p)

        d = i - done_lag

        @pl.when(jnp.logical_and(jnp.logical_and(d >= 0, d < pieces), place != 2))
        def _():
            finish(d)

    wait_x(0)

    @pl.loop(0, HEAD)
    def _(k):
        gate_copy(k).wait()
        up_copy(k).wait()

        @pl.when(k + AHEAD < HEAD)
        def _():
            gate_copy(k + AHEAD).start()
            up_copy(k + AHEAD).start()

        @pl.when(k == DOWN_AT)
        def _():
            for t in range(tiles):
                down_copy(t).start()
            fetch_x(1)

        xs = x_buf[0, :, depth_slice(k)]
        gate = dot(xs, gate_w[depth_slice(k)])
        up = dot(xs, up_w[depth_slice(k)])

        @pl.when(k == 0)
        def _():
            first_gate[...] = gate
            first_up[...] = up

        @pl.when(k > 0)
        def _():
            first_gate[...] += gate
            first_up[...] += up

    hidden[0] = activate(first_gate[...], first_up[...])
    pl.semaphore_wait(barrier, jnp.where(inner, 3, 2))

    @pl.loop(0, pieces + LONGEST)
    def _(i):
        c, t = i // tiles, lax.rem(i, tiles)

        @pl.when(i < pieces)
        def _():
            @pl.when(c == 0)
            def _():
                down_copy(t).wait()

            @pl.when(jnp.logical_and(t == 0, c + 2 < chunks))
            def _():
                fetch_x(c + 2)

            @pl.when(jnp.logical_and(t == 0, c + 1 < chunks))
            def _():
                wait_x(c + 1)

            terms(c, t)

            @pl.when(c + 1 < chunks)
            def _():
                project(c + 1, t)

        trail(i)

    for k in range(STAGE):
        stage_copy(pieces - STAGE + k).wait_send()
    pltpu.make_async_copy(sums, sums, sum_sem).wait()

    @pl.when(place == 2)
    def _():
        pltpu.make_async_copy(sums, sums, spread_sem).wait()

    @pl.when(place == 1)
    def _():
        pltpu.make_async_copy(high, high, pass_sem).wait()

    pltpu.make_async_copy(sums, sums, y_sem).wait()
    pltpu.make_async_copy(sums, sums, give_sem).wait()
    pltpu.make_async_copy(sums, sums, take_sem).wait()


def put_out(y_vmem, y_hbm, sem):
    rows = y_vmem.shape[0] // OUT_COPIES
    for k in range(OUT_COPIES):
        part = pl.ds(k * rows, rows)
        pltpu.make_async_copy(y_vmem.at[part], y_hbm.at[part], sem).start()
    pltpu.make_async_copy(y_vmem, y_hbm, sem).wait()


def block(x, w_gate, w_up, w_down, chunk=CHUNK, tiles=TILES):
    rows, depth = x.shape
    units = w_gate.shape[1]
    pieces = rows // 2 // chunk * tiles
    piece = (chunk, depth // tiles)
    messages = pieces * PARTS
    buffers = pltpu.VMEM((messages, chunk, depth // tiles // PARTS), jnp.bfloat16)
    dma = pltpu.SemaphoreType.DMA
    anywhere = pl.BlockSpec(memory_space=pl.ANY)
    y = pl.pallas_call(
        functools.partial(kernel, chunk, tiles),
        out_shape=pltpu.VMEM((rows, depth), jnp.bfloat16),
        in_specs=[anywhere] * 4,
        out_specs=anywhere,
        scratch_shapes=[
            pltpu.VMEM((depth, units), jnp.bfloat16),
            pltpu.VMEM((depth, units), jnp.bfloat16),
            pltpu.VMEM((units, depth), jnp.bfloat16),
            pltpu.VMEM((2, 2 * chunk, depth), jnp.bfloat16),
            pltpu.VMEM((2, 2 * chunk, units), jnp.bfloat16),
            pltpu.VMEM((2 * chunk, units), jnp.float32),
            pltpu.VMEM((2 * chunk, units), jnp.float32),
            pltpu.VMEM((RING,) + piece, jnp.float32),
            pltpu.VMEM((STAGE,) + piece, jnp.bfloat16),
            pltpu.VMEM((pieces,) + piece, jnp.bfloat16), buffers, buffers, buffers,
            dma((2,)), dma((HEAD,)), dma((HEAD,)), dma((tiles,)), dma((STAGE,)),
            dma((pieces,)), dma((messages,)), dma((messages,)),
            dma, dma, dma, dma, dma, dma,
        ],
        compiler_params=pltpu.CompilerParams(
            collective_id=0, has_side_effects=True, vmem_limit_bytes=54_000_000
        ),
    )(x, w_gate, w_up, w_down)
    return pl.pallas_call(
        put_out,
        out_shape=jax.ShapeDtypeStruct((rows, depth), jnp.bfloat16),
        in_specs=[anywhere],
        out_specs=anywhere,
        scratch_shapes=[dma],
        compiler_params=pltpu.CompilerParams(vmem_limit_bytes=OUT_LIMIT),
    )(y)


def solution(mesh):
    return jax.shard_map(
        block,
        mesh=mesh,
        in_specs=(P("dp", None), P(None, "tp"), P(None, "tp"), P("tp", None)),
        out_specs=P("dp", None),
        check_vma=False,
    )
```

```python
import functools

import jax
import jax.numpy as jnp
from jax import lax
from jax.experimental import pallas as pl
from jax.experimental.pallas import tpu as pltpu
from jax.sharding import PartitionSpec as P

MESH = pl.DeviceIdType.MESH
CHIPS = 4
CHUNK = 64
TILES = 4
RING = 16
STAGE = 4
OUT_COPIES = 16
OUT_LIMIT = 1_000_000
SUM_LAG = ((0, 2, 5, 4), (0, 2, 5, 3))
DONE_LAG = ((24, 6, 24, 24), (24, 6, 24, 24))
PARTS = 1
HEAD = 6
AHEAD = 4
DOWN_AT = 3


def by_place(core, place, rows):
    result = jnp.int32(rows[-1][-1])
    for k, row in enumerate(rows):
        for j, value in enumerate(row):
            result = jnp.where(jnp.logical_and(core == k, place == j), jnp.int32(value), result)
    return result


LONGEST = max(max(row) for row in SUM_LAG + DONE_LAG)


def kernel(
    chunk, tiles, x_hbm, gate_hbm, up_hbm, down_hbm, y_hbm,
    gate_w, up_w, down_w, x_buf, hidden, first_gate, first_up, own, stage, theirs, low, high, sums,
    x_sem, gate_sem, up_sem, down_sem, stage_sem, theirs_sem, low_sem, high_sem,
    sum_sem, spread_sem, pass_sem, y_sem, give_sem, take_sem,
):
    rows, depth = x_hbm.shape
    units = gate_hbm.shape[1]
    half = rows // 2
    chunks = half // chunk
    pieces = chunks * tiles
    unit_tile = units // tiles
    col_tile = depth // tiles

    me = lax.axis_index("tp")
    chip, core = me // 2, me % 2
    place = jnp.where(core == 1, chip, CHIPS - 1 - chip)

    def at_place(k):
        return {"tp": jnp.where(core == 1, k, CHIPS - 1 - k) * 2 + core}

    other = {"tp": me + 1 - 2 * core}
    before, after = at_place(place - 1), at_place(place + 1)
    inner = jnp.logical_or(place == 1, place == 2)

    barrier = pltpu.get_barrier_semaphore()
    pl.semaphore_signal(barrier, inc=1, device_id=other, device_id_type=MESH)

    @pl.when(place > 0)
    def _():
        pl.semaphore_signal(barrier, inc=1, device_id=before, device_id_type=MESH)

    @pl.when(place < CHIPS - 1)
    def _():
        pl.semaphore_signal(barrier, inc=1, device_id=after, device_id_type=MESH)

    def x_rows(which, c):
        return x_hbm.at[pl.ds(pl.multiple_of(which * half + c * chunk, chunk), chunk), :]

    def fetch_x(c):
        slot = lax.rem(c, 2)
        pltpu.make_async_copy(x_rows(core, c), x_buf.at[slot, pl.ds(0, chunk)], x_sem.at[slot]).start()
        pltpu.make_async_copy(x_rows(1 - core, c), x_buf.at[slot, pl.ds(chunk, chunk)], x_sem.at[slot]).start()

    def wait_x(c):
        slot = lax.rem(c, 2)
        pltpu.make_async_copy(x_hbm.at[pl.ds(0, 2 * chunk), :], x_buf.at[slot], x_sem.at[slot]).wait()

    depth_tile = depth // HEAD
    part_tile = col_tile // PARTS

    def unit_slice(t):
        return pl.ds(pl.multiple_of(t * unit_tile, unit_tile), unit_tile)

    def depth_slice(k):
        return pl.ds(pl.multiple_of(k * depth_tile, depth_tile), depth_tile)

    def col_slice(t):
        return pl.ds(pl.multiple_of(t * col_tile, col_tile), col_tile)

    def gate_copy(k):
        return pltpu.make_async_copy(gate_hbm.at[depth_slice(k)], gate_w.at[depth_slice(k)], gate_sem.at[k])

    def up_copy(k):
        return pltpu.make_async_copy(up_hbm.at[depth_slice(k)], up_w.at[depth_slice(k)], up_sem.at[k])

    def down_copy(t):
        return pltpu.make_async_copy(down_hbm.at[:, col_slice(t)], down_w.at[:, col_slice(t)], down_sem.at[t])

    def dot(a, b):
        return jnp.dot(a, b, preferred_element_type=jnp.float32)

    def activate(gate, up):
        return (jax.nn.silu(gate) * up).astype(jnp.bfloat16)

    def project(c, t):
        slot = lax.rem(c, 2)
        xs = x_buf[slot]
        hidden[slot, :, unit_slice(t)] = activate(dot(xs, gate_w[:, unit_slice(t)]), dot(xs, up_w[:, unit_slice(t)]))

    fetch_x(0)
    @pl.loop(0, AHEAD)
    def _(k):
        gate_copy(k).start()
        up_copy(k).start()

    def stage_copy(i):
        slot = lax.rem(i, STAGE)
        return pltpu.make_async_remote_copy(
            src_ref=stage.at[slot], dst_ref=theirs.at[i], send_sem=stage_sem.at[slot], recv_sem=theirs_sem.at[i],
            device_id=other, device_id_type=MESH,
        )

    def terms(c, t):
        i = c * tiles + t
        term = dot(hidden[lax.rem(c, 2)], down_w[:, col_slice(t)])

        @pl.when(i >= STAGE)
        def _():
            stage_copy(i - STAGE).wait_send()

        stage[lax.rem(i, STAGE)] = term[chunk:].astype(jnp.bfloat16)
        stage_copy(i).start()
        own[lax.rem(i, RING)] = term[:chunk]

    def low_copy(p):
        return pltpu.make_async_remote_copy(
            src_ref=sums.at[p], dst_ref=low.at[p], send_sem=sum_sem, recv_sem=low_sem.at[p],
            device_id=after, device_id_type=MESH,
        )

    def high_copy(p):
        return pltpu.make_async_remote_copy(
            src_ref=sums.at[p], dst_ref=high.at[p], send_sem=sum_sem, recv_sem=high_sem.at[p],
            device_id=before, device_id_type=MESH,
        )

    def spread_copy(p):
        return pltpu.make_async_remote_copy(
            src_ref=sums.at[p], dst_ref=high.at[p], send_sem=spread_sem, recv_sem=high_sem.at[p],
            device_id=after, device_id_type=MESH,
        )

    def pass_copy(p):
        return pltpu.make_async_remote_copy(
            src_ref=high.at[p], dst_ref=high.at[p], send_sem=pass_sem, recv_sem=high_sem.at[p],
            device_id=before, device_id_type=MESH,
        )

    def deliver(src, m):
        p = m // PARTS
        c, column = p // tiles, lax.rem(p, tiles) * col_tile + lax.rem(m, PARTS) * part_tile
        block = y_hbm.at[
            pl.ds(pl.multiple_of(core * half + c * chunk, chunk), chunk),
            pl.ds(pl.multiple_of(column, part_tile), part_tile),
        ]
        pltpu.make_async_remote_copy(
            src_ref=src, dst_ref=block, send_sem=give_sem, recv_sem=take_sem, device_id=other, device_id_type=MESH,
        ).start()
        pltpu.make_async_copy(src, block, y_sem).start()

    def combine(p):
        pltpu.make_async_copy(theirs.at[p], theirs.at[p], theirs_sem.at[p]).wait()
        for part in range(PARTS):
            combine_part(p, part)

    def combine_part(p, part):
        m = p * PARTS + part
        columns = slice(part * part_tile, (part + 1) * part_tile)

        def here():
            return own[lax.rem(p, RING), :, columns] + theirs[p, :, columns].astype(jnp.float32)

        @pl.when(jnp.logical_not(inner))
        def _():
            sums[m] = here().astype(jnp.bfloat16)

        @pl.when(inner)
        def _():
            pltpu.make_async_copy(low.at[m], low.at[m], low_sem.at[m]).wait()

        @pl.when(place == 1)
        def _():
            sums[m] = (here() + low[m].astype(jnp.float32)).astype(jnp.bfloat16)

        @pl.when(place == 2)
        def _():
            pltpu.make_async_copy(high.at[m], high.at[m], high_sem.at[m]).wait()
            sums[m] = (here() + low[m].astype(jnp.float32) + high[m].astype(jnp.float32)).astype(jnp.bfloat16)

        @pl.when(place < 2)
        def _():
            low_copy(m).start()

        @pl.when(place >= 2)
        def _():
            high_copy(m).start()

        @pl.when(place == 2)
        def _():
            spread_copy(m).start()
            deliver(sums.at[m], m)

    def finish(p):
        for part in range(PARTS):
            m = p * PARTS + part
            pltpu.make_async_copy(high.at[m], high.at[m], high_sem.at[m]).wait()

            @pl.when(place == 1)
            def _():
                pass_copy(m).start()

            deliver(high.at[m], m)

    sum_lag = by_place(core, place, SUM_LAG)
    done_lag = by_place(core, place, DONE_LAG)

    def trail(i):
        p = i - sum_lag

        @pl.when(jnp.logical_and(p >= 0, p < pieces))
        def _():
            combine(p)

        d = i - done_lag

        @pl.when(jnp.logical_and(jnp.logical_and(d >= 0, d < pieces), place != 2))
        def _():
            finish(d)

    wait_x(0)

    @pl.loop(0, HEAD)
    def _(k):
        gate_copy(k).wait()
        up_copy(k).wait()

        @pl.when(k + AHEAD < HEAD)
        def _():
            gate_copy(k + AHEAD).start()
            up_copy(k + AHEAD).start()

        @pl.when(k == DOWN_AT)
        def _():
            for t in range(tiles):
                down_copy(t).start()
            fetch_x(1)

        xs = x_buf[0, :, depth_slice(k)]
        gate = dot(xs, gate_w[depth_slice(k)])
        up = dot(xs, up_w[depth_slice(k)])

        @pl.when(k == 0)
        def _():
            first_gate[...] = gate
            first_up[...] = up

        @pl.when(k > 0)
        def _():
            first_gate[...] += gate
            first_up[...] += up

    hidden[0] = activate(first_gate[...], first_up[...])
    pl.semaphore_wait(barrier, jnp.where(inner, 3, 2))

    @pl.loop(0, pieces + LONGEST)
    def _(i):
        c, t = i // tiles, lax.rem(i, tiles)

        @pl.when(i < pieces)
        def _():
            @pl.when(c == 0)
            def _():
                down_copy(t).wait()

            @pl.when(jnp.logical_and(t == 0, c + 2 < chunks))
            def _():
                fetch_x(c + 2)

            @pl.when(jnp.logical_and(t == 0, c + 1 < chunks))
            def _():
                wait_x(c + 1)

            terms(c, t)

            @pl.when(c + 1 < chunks)
            def _():
                project(c + 1, t)

        trail(i)

    for k in range(STAGE):
        stage_copy(pieces - STAGE + k).wait_send()
    pltpu.make_async_copy(sums, sums, sum_sem).wait()

    @pl.when(place == 2)
    def _():
        pltpu.make_async_copy(sums, sums, spread_sem).wait()

    @pl.when(place == 1)
    def _():
        pltpu.make_async_copy(high, high, pass_sem).wait()

    pltpu.make_async_copy(sums, sums, y_sem).wait()
    pltpu.make_async_copy(sums, sums, give_sem).wait()
    pltpu.make_async_copy(sums, sums, take_sem).wait()


def put_out(y_vmem, y_hbm, sem):
    rows = y_vmem.shape[0] // OUT_COPIES
    for k in range(OUT_COPIES):
        part = pl.ds(k * rows, rows)
        pltpu.make_async_copy(y_vmem.at[part], y_hbm.at[part], sem).start()
    pltpu.make_async_copy(y_vmem, y_hbm, sem).wait()


def block(x, w_gate, w_up, w_down, chunk=CHUNK, tiles=TILES):
    rows, depth = x.shape
    units = w_gate.shape[1]
    pieces = rows // 2 // chunk * tiles
    piece = (chunk, depth // tiles)
    messages = pieces * PARTS
    buffers = pltpu.VMEM((messages, chunk, depth // tiles // PARTS), jnp.bfloat16)
    dma = pltpu.SemaphoreType.DMA
    anywhere = pl.BlockSpec(memory_space=pl.ANY)
    y = pl.pallas_call(
        functools.partial(kernel, chunk, tiles),
        out_shape=pltpu.VMEM((rows, depth), jnp.bfloat16),
        in_specs=[anywhere] * 4,
        out_specs=anywhere,
        scratch_shapes=[
            pltpu.VMEM((depth, units), jnp.bfloat16),
            pltpu.VMEM((depth, units), jnp.bfloat16),
            pltpu.VMEM((units, depth), jnp.bfloat16),
            pltpu.VMEM((2, 2 * chunk, depth), jnp.bfloat16),
            pltpu.VMEM((2, 2 * chunk, units), jnp.bfloat16),
            pltpu.VMEM((2 * chunk, units), jnp.float32),
            pltpu.VMEM((2 * chunk, units), jnp.float32),
            pltpu.VMEM((RING,) + piece, jnp.float32),
            pltpu.VMEM((STAGE,) + piece, jnp.bfloat16),
            pltpu.VMEM((pieces,) + piece, jnp.bfloat16), buffers, buffers, buffers,
            dma((2,)), dma((HEAD,)), dma((HEAD,)), dma((tiles,)), dma((STAGE,)),
            dma((pieces,)), dma((messages,)), dma((messages,)),
            dma, dma, dma, dma, dma, dma,
        ],
        compiler_params=pltpu.CompilerParams(
            collective_id=0, has_side_effects=True, vmem_limit_bytes=54_000_000
        ),
    )(x, w_gate, w_up, w_down)
    return pl.pallas_call(
        put_out,
        out_shape=jax.ShapeDtypeStruct((rows, depth), jnp.bfloat16),
        in_specs=[anywhere],
        out_specs=anywhere,
        scratch_shapes=[dma],
        compiler_params=pltpu.CompilerParams(vmem_limit_bytes=OUT_LIMIT),
    )(y)


def solution(mesh):
    return jax.shard_map(
        block,
        mesh=mesh,
        in_specs=(P("dp", None), P(None, "tp"), P(None, "tp"), P("tp", None)),
        out_specs=P("dp", None),
        check_vma=False,
    )
```
